128 devices in a mesh: img: 16 (over z, y_hi, core), feat: 8 (over y_lo, x).
Axes of the slice: x: 4, y: 4 (y_hi: 2, y_lo: 2; y = y_hi * 2 + y_lo), z: 4, core: 2. Of those that a mesh axis runs over, the one named last changes fastest.
Arguments:
- features: bfloat16 [16384, 32768], P('img', 'feat'), may hold values from -0.055242717 to 0.055242717
- weights: bfloat16 [512, 32768], P('img', 'feat'), may hold values from -20 to 20
- direction: bfloat16 [512, 32768], P('img', 'feat'), may hold values from -6 to 6
Outputs:
- hessian_product: float32 [512, 32768], P('img', 'feat')
The draws below stay inside these ranges and needn't reach their ends.
All inputs are finite; a program needn't handle non-finite values.
Results may differ from the reference program's by a relative error of at most 0.0024.
Values may be sent and summed in bfloat16 or wider, within the bound.
A program may use at most 64 MiB of HBM per device.

```python
import jax
import jax.numpy as jnp
from jax import lax

FEATS = 32768
CLASSES = 512
ROWS_DEV = 1024
IMAGES = 16384


def draw_features(key, part):
    first = jax.random.fold_in(key, 11)
    base = jnp.clip(jax.random.normal(first, (IMAGES, FEATS), jnp.float32), -6.0, 6.0)
    return (jnp.clip(base, -10.0, 10.0) * FEATS ** (-0.5)).astype(jnp.bfloat16)


def draw_weights(key, part):
    first = jax.random.fold_in(key, 21)
    base = 2.0 * jnp.clip(jax.random.normal(first, (CLASSES, FEATS), jnp.float32), -6.0, 6.0)
    return jnp.clip(base, -20.0, 20.0).astype(jnp.bfloat16)


def block_levels(rng, extent, shards, smallest, top_value):
    loudness, own = 1.0, jax.random.fold_in(rng, 6)
    for position, blocks in shards:
        steps = jnp.exp(jax.random.uniform(jax.random.fold_in(own, position), (blocks,), jnp.float32, smallest / len(shards), top_value / len(shards)))
        loudness = loudness * jnp.repeat(steps, extent[position] // blocks).reshape([-1 if axis == position else 1 for axis in range(len(extent))])
    return loudness


def centred(rng, shape, width, most, shards=(), held_as=jnp.bfloat16):
    level = block_levels(rng, shape, shards, -0.22, 0.18) if shards else 1.0
    array = jax.random.normal(rng, shape, jnp.float32) * width * level
    return jnp.minimum(jnp.maximum(array, -most), most).astype(held_as)


def setup_inputs(seed: int = 0) -> dict:
    seeds = jax.random.split(jax.random.key(seed), 4)
    return {
        "features": draw_features(jax.random.fold_in(seeds[3], 71), 0),
        "weights": draw_weights(jax.random.fold_in(seeds[3], 71), 0),
        "direction": centred(seeds[2], (CLASSES, FEATS), 1.0, 6.0, ((0, 16), (1, 8))),
    }


def reference(features, weights, direction):
    wide_w = weights.astype(jnp.float32)
    wide_v = direction.astype(jnp.float32)
    blocks = features.reshape(IMAGES // ROWS_DEV, ROWS_DEV, FEATS)

    def step(total, block):
        rows = block.astype(jnp.float32)
        scores = jnp.dot(rows, wide_w.T, preferred_element_type=jnp.float32)
        slopes = jnp.dot(rows, wide_v.T, preferred_element_type=jnp.float32)
        prob = jax.nn.sigmoid(scores)
        curvature = (prob * (1.0 - prob) * slopes).astype(jnp.bfloat16).astype(jnp.float32)
        return total + jnp.dot(curvature.T, rows, preferred_element_type=jnp.float32), None

    total, unused = lax.scan(step, jnp.zeros((CLASSES, FEATS), jnp.float32), blocks)
    return 4.0 * total
```

```python
import jax
import jax.numpy as jnp
from jax import lax
from jax.experimental import pallas as pl
from jax.experimental.pallas import tpu as pltpu
from jax.sharding import PartitionSpec as P

ZS, YHS, CORES, YLS, XS = 4, 2, 2, 2, 4
CHUNKS = 4
COPIES = 31
PERIOD = 11.0
STAGES = (
    ("gather_start", 0.0),
    ("gather_second", 4.0),
    ("gather_forward", 8.0),
    ("gather_last", 12.0),
    ("scores", 14.0),
    ("scores_second", 20.0),
    ("scores_pair", 25.0),
    ("curvature", 28.0),
    ("curvature_second", 30.0),
    ("curvature_forward", 32.0),
    ("terms", 34.0),
    ("terms_first", 39.0),
    ("terms_second", 42.0),
    ("terms_pair", 45.0),
    ("terms_last", 48.0),
)


def order():
    events = []
    for place, (name, at) in enumerate(STAGES):
        for k in range(CHUNKS):
            lead = 0.0
            if place == 0:
                lead = -PERIOD + 3.0 if k else 0.0
            events.append((at + PERIOD * k + lead, place, k, name))
    return [(name, k) for _, _, k, name in sorted(events)]


def kernel(
    feat_hbm, w_hbm, d_hbm, out_ref,
    feat, w_ref, d_ref, gath, part, r1, r2, r3, curv, hess, r4,
    s5, r5, s6, r6, s7, r7,
    load, send, recv,
):
    f32, bf16 = jnp.float32, jnp.bfloat16
    img, col = lax.axis_index("img"), lax.axis_index("feat")
    core = lax.rem(img, CORES)
    yh = lax.rem(img // CORES, YHS)
    z = img // (CORES * YHS)
    x = lax.rem(col, XS)
    yl = col // XS
    z_up, z_down, z_far = lax.rem(z + 1, ZS), lax.rem(z + 3, ZS), lax.rem(z + 2, ZS)
    x_up, x_down, x_far = lax.rem(x + 1, XS), lax.rem(x + 3, XS), lax.rem(x + 2, XS)

    def at(z=z, yh=yh, core=core, yl=yl, x=x):
        return {"img": (z * YHS + yh) * CORES + core, "feat": yl * XS + x}

    to_z_up, to_z_down = at(z=z_up), at(z=z_down)
    to_x_up, to_x_down = at(x=x_up), at(x=x_down)
    to_yh, to_core, to_yl = at(yh=1 - yh), at(core=1 - core), at(yl=1 - yl)

    loads = [
        pltpu.make_async_copy(w_hbm, w_ref, load.at[0]),
        pltpu.make_async_copy(d_hbm, d_ref, load.at[1]),
        pltpu.make_async_copy(feat_hbm, feat, load.at[2]),
    ]
    for one in loads:
        one.start()
    barrier = pltpu.get_barrier_semaphore()
    partners = (to_z_up, to_z_down, to_x_up, to_x_down, to_yh, to_core, to_yl)
    for partner in partners:
        pl.semaphore_signal(
            barrier, inc=1, device_id=partner, device_id_type=pl.DeviceIdType.MESH
        )

    started = {}

    def push(k, number, src, dst, device):
        one = pltpu.make_async_remote_copy(
            src_ref=src,
            dst_ref=dst,
            send_sem=send.at[k, number],
            recv_sem=recv.at[k, number],
            device_id=device,
            device_id_type=pl.DeviceIdType.MESH,
        )
        one.start()
        started[k, number] = one

    def arrived(k, *numbers):
        for number in numbers:
            started[k, number].wait_recv()

    def same(k, number, ref, device):
        push(k, number, ref, ref, device)

    class Steps:
        def pack(k):
            rows = pl.ds(8 * k, 8)
            both = jnp.concatenate(
                (w_ref[...].astype(f32)[8 * k : 8 * k + 8], d_ref[...].astype(f32)[8 * k : 8 * k + 8]),
                axis=0,
            )
            gath[k, z, yh, core] = both.astype(bf16)

        def gather_start(k):
            mine = gath.at[k, z, yh, core]
            same(k, 0, mine, to_yh)
            same(k, 1, mine, to_z_up)
            same(k, 2, mine, to_z_down)
            same(k, 7, mine, to_core)

        def gather_second(k):
            arrived(k, 0)
            theirs = gath.at[k, z, 1 - yh, core]
            same(k, 3, theirs, to_z_up)
            same(k, 4, theirs, to_z_down)
            same(k, 8, theirs, to_core)

        def gather_forward(k):
            arrived(k, 1, 3)
            same(k, 5, gath.at[k, z_down, 0, core], to_z_up)
            arrived(k, 2, 4)
            same(k, 6, gath.at[k, z_up, 1, core], to_z_down)
            same(k, 9, gath.at[k, z_down, :, core], to_core)
            same(k, 10, gath.at[k, z_up, :, core], to_core)

        def gather_last(k):
            arrived(k, 5)
            same(k, 11, gath.at[k, z_far, 0, core], to_core)
            arrived(k, 6)
            same(k, 12, gath.at[k, z_far, 1, core], to_core)

        def scores(k):
            if k == 0:
                loads[2].wait()
            arrived(k, 7, 8, 9, 10, 11, 12)
            rows, depth = feat.shape
            tile = 256

            @pl.loop(0, rows // tile)
            def _(n):
                here = pl.ds(pl.multiple_of(n * tile, tile), tile)
                both = lax.dot_general(
                    gath[k].reshape(-1, depth),
                    feat[here, :],
                    (((1,), (1,)), ((), ())),
                    preferred_element_type=f32,
                )
                part[k, :, :, :, here] = both.reshape(YLS, XS, -1, tile)

            push(k, 13, part.at[k, 0, x_far], r1.at[k, 0], to_x_up)
            push(k, 14, part.at[k, 1, x_far], r1.at[k, 1], to_x_down)

        def scores_second(k):
            arrived(k, 13)
            part[k, 0, x_up] += r1[k, 0]
            push(k, 15, part.at[k, :, x_up], r2.at[k, 0], to_x_up)
            arrived(k, 14)
            part[k, 1, x_down] += r1[k, 1]
            push(k, 16, part.at[k, :, x_down], r2.at[k, 1], to_x_down)

        def scores_pair(k):
            arrived(k, 15, 16)
            part[k, 1 - yl, x] += r2[k, 0, 1 - yl] + r2[k, 1, 1 - yl]
            push(k, 17, part.at[k, 1 - yl, x], r3.at[k], to_yl)
            part[k, yl, x] += r2[k, 0, yl] + r2[k, 1, yl]

        def curvature(k):
            arrived(k, 17)
            total = part[k, yl, x] + r3[k]
            pair = total.reshape(2, 2, 8, total.shape[-1])
            prob = jax.nn.sigmoid(pair[:, 0])
            value = prob * (1.0 - prob) * pair[:, 1]
            curv[k, yl, x] = value.reshape(16, value.shape[-1]).astype(bf16)
            mine = curv.at[k, yl, x]
            same(k, 18, mine, to_yl)
            same(k, 19, mine, to_x_up)
            same(k, 20, mine, to_x_down)

        def curvature_second(k):
            arrived(k, 18)
            theirs = curv.at[k, 1 - yl, x]
            same(k, 21, theirs, to_x_up)
            same(k, 22, theirs, to_x_down)

        def curvature_forward(k):
            arrived(k, 19, 21)
            same(k, 23, curv.at[k, 0, x_down], to_x_up)
            arrived(k, 20, 22)
            same(k, 24, curv.at[k, 1, x_up], to_x_down)

        def terms(k):
            arrived(k, 23, 24)
            rows, depth = feat.shape
            tile = 512

            @pl.loop(0, depth // tile)
            def _(n):
                here = pl.ds(pl.multiple_of(n * tile, tile), tile)
                term = jnp.dot(
                    curv[k].reshape(-1, rows), feat[:, here], preferred_element_type=f32
                )
                hess[k, :, :, :, :, here] = term.reshape(ZS, YHS, CORES, 8, tile)

            push(k, 25, hess.at[k, :, :, 1 - core], r4.at[k], to_core)

        def chip(k, place):
            both = hess[k, place, :, core] + r4[k, place]
            return both.reshape(16, both.shape[-1])

        def terms_first(k):
            arrived(k, 25)
            s5[k] = Steps.chip(k, z_far).astype(bf16)
            half = s5.shape[-1] // 2
            push(k, 26, s5.at[k, :, pl.ds(0, half)], r5.at[k, 0], to_z_up)
            push(k, 27, s5.at[k, :, pl.ds(half, half)], r5.at[k, 1], to_z_down)

        def terms_second(k):
            half = s5.shape[-1] // 2
            arrived(k, 26)
            up = Steps.chip(k, z_up)
            s6[k, 0, :, :half] = (up[:, :half] + r5[k, 0].astype(f32)).astype(bf16)
            s6[k, 0, :, half:] = up[:, half:].astype(bf16)
            push(k, 28, s6.at[k, 0], r6.at[k, 0], to_z_up)
            arrived(k, 27)
            down = Steps.chip(k, z_down)
            s6[k, 1, :, :half] = down[:, :half].astype(bf16)
            s6[k, 1, :, half:] = (down[:, half:] + r5[k, 1].astype(f32)).astype(bf16)
            push(k, 29, s6.at[k, 1], r6.at[k, 1], to_z_down)

        def terms_pair(k):
            arrived(k, 28, 29)
            own = Steps.chip(k, z) + r6[k, 0].astype(f32) + r6[k, 1].astype(f32)
            half = own.shape[-1] // 2
            first = yh == 0
            mine = jnp.where(first, own[:8], own[8:])
            theirs = jnp.where(first, own[8:], own[:8])
            s7[k] = jnp.concatenate((theirs[:, :half], theirs[:, half:]), axis=0).astype(bf16)
            push(k, 30, s7.at[k], r7.at[k], to_yh)
            out_ref[8 * k : 8 * k + 8, :] = mine

        def terms_last(k):
            arrived(k, 30)
            other = r7[k].astype(f32)
            half = other.shape[-1]
            rows = slice(8 * k, 8 * k + 8)
            out_ref[rows, :half] = 4.0 * (out_ref[rows, :half] + other[:8])
            out_ref[rows, half:] = 4.0 * (out_ref[rows, half:] + other[8:])

    loads[0].wait()
    loads[1].wait()
    for k in range(CHUNKS):
        Steps.pack(k)
    pl.semaphore_wait(barrier, len(partners))
    for name, k in order():
        getattr(Steps, name)(k)
    for one in started.values():
        one.wait_send()


def body(features, weights, direction):
    rows, depth = features.shape
    mine = weights.shape[0]
    K = CHUNKS
    f32, bf16 = jnp.float32, jnp.bfloat16
    vmem = pltpu.VMEM
    return pl.pallas_call(
        kernel,
        out_shape=jax.ShapeDtypeStruct((mine, depth), f32),
        in_specs=[pl.BlockSpec(memory_space=pl.ANY)] * 3,
        out_specs=pl.BlockSpec(memory_space=vmem),
        scratch_shapes=[
            vmem((rows, depth), bf16),
            vmem((mine, depth), bf16),
            vmem((mine, depth), bf16),
            vmem((K, ZS, YHS, CORES, 16, depth), bf16),
            vmem((K, YLS, XS, 32, rows), f32),
            vmem((K, 2, 32, rows), f32),
            vmem((K, 2, YLS, 32, rows), f32),
            vmem((K, 32, rows), f32),
            vmem((K, YLS, XS, 16, rows), bf16),
            vmem((K, ZS, YHS, CORES, 8, depth), f32),
            vmem((K, ZS, YHS, 8, depth), f32),
            vmem((K, 16, depth), bf16),
            vmem((K, 2, 16, depth // 2), bf16),
            vmem((K, 2, 16, depth), bf16),
            vmem((K, 2, 16, depth), bf16),
            vmem((K, 16, depth // 2), bf16),
            vmem((K, 16, depth // 2), bf16),
            pltpu.SemaphoreType.DMA((3,)),
            pltpu.SemaphoreType.DMA((K, COPIES)),
            pltpu.SemaphoreType.DMA((K, COPIES)),
        ],
        compiler_params=pltpu.CompilerParams(
            collective_id=0, has_side_effects=True, vmem_limit_bytes=62 * 2**20
        ),
    )(features, weights, direction)


def solution(mesh):
    placed = (P("img", "feat"), P("img", "feat"), P("img", "feat"))
    return jax.shard_map(
        body, mesh=mesh, in_specs=placed, out_specs=P("img", "feat"), check_vma=False
    )
```

```python
import jax
import jax.numpy as jnp
from jax import lax
from jax.experimental import pallas as pl
from jax.experimental.pallas import tpu as pltpu
from jax.sharding import PartitionSpec as P

ZS, YHS, CORES, YLS, XS = 4, 2, 2, 2, 4
CHUNKS = 4
PIECES = 2
COPIES = 31
NAMES = (
    "gather_start", "gather_second", "gather_forward", "gather_last",
    "scores", "scores_second", "scores_pair", "curvature", "", "",
    "terms", "terms_first", "", "terms_pair", "terms_last",
)
ORDER = (
    (0, 0, 0), (0, 0, 1), (0, 1, 0), (1, 0, 0), (1, 0, 1), (0, 1, 1), (2, 0, 0),
    (2, 0, 1), (3, 0, 0), (1, 1, 1), (0, 2, 0), (1, 1, 0), (0, 2, 1), (3, 0, 1),
    (4, 0, 0), (2, 1, 1), (5, 0, 0), (2, 1, 0), (1, 2, 1), (0, 3, 0), (3, 1, 1),
    (0, 3, 1), (1, 2, 0), (3, 1, 0), (5, 0, 1), (6, 0, 0), (4, 1, 0), (1, 3, 1),
    (6, 0, 1), (2, 2, 1), (7, 0, 0), (5, 1, 0), (2, 2, 0), (3, 2, 1), (5, 1, 1),
    (1, 3, 0), (7, 0, 1), (3, 2, 0), (6, 1, 0), (2, 3, 0), (2, 3, 1), (4, 2, 0),
    (7, 1, 0), (3, 3, 1), (6, 1, 1), (5, 2, 0), (3, 3, 0), (10, 0, 0), (7, 1, 1),
    (4, 3, 0), (6, 2, 0), (5, 2, 1), (11, 0, 1), (11, 0, 0), (5, 3, 0), (10, 1, 0),
    (11, 1, 0), (5, 3, 1), (7, 2, 0), (6, 2, 1), (6, 3, 0), (7, 2, 1), (6, 3, 1),
    (13, 0, 0), (7, 3, 0), (7, 3, 1), (11, 1, 1), (10, 2, 0), (11, 2, 0), (13, 0, 1),
    (13, 1, 1), (11, 2, 1), (10, 3, 0), (11, 3, 0), (14, 0, 1), (13, 2, 0), (13, 1, 0),
    (14, 1, 1), (11, 3, 1), (13, 3, 0), (13, 2, 1), (13, 3, 1), (14, 3, 0), (14, 2, 0),
    (14, 1, 0), (14, 2, 1), (14, 0, 0), (14, 3, 1),
)


def kernel(
    feat_hbm, w_hbm, d_hbm, out_hbm,
    feat, w_ref, d_ref, gath, part, r1, r2, r3, curv, hess, r4,
    zs, zr, ys, yr, out,
    load, store, send, recv,
):
    f32, bf16 = jnp.float32, jnp.bfloat16
    mesh_ids = pl.DeviceIdType.MESH
    img, col = lax.axis_index("img"), lax.axis_index("feat")
    core = lax.rem(img, CORES)
    yh = lax.rem(img // CORES, YHS)
    z = img // (CORES * YHS)
    x = lax.rem(col, XS)
    yl = col // XS
    z_up, z_down, z_far = lax.rem(z + 1, ZS), lax.rem(z + 3, ZS), lax.rem(z + 2, ZS)
    x_up, x_down, x_far = lax.rem(x + 1, XS), lax.rem(x + 3, XS), lax.rem(x + 2, XS)

    def at(z=z, yh=yh, core=core, yl=yl, x=x):
        return {"img": (z * YHS + yh) * CORES + core, "feat": yl * XS + x}

    to_z_up, to_z_down, to_z_far = at(z=z_up), at(z=z_down), at(z=z_far)
    to_x_up, to_x_down, to_x_far = at(x=x_up), at(x=x_down), at(x=x_far)
    to_yh, to_core, to_yl = at(yh=1 - yh), at(core=1 - core), at(yl=1 - yl)
    across = [at(yl=1 - yl, x=one) for one in (x_up, x_down, x_far)]

    loads = [
        pltpu.make_async_copy(w_hbm, w_ref, load.at[0]),
        pltpu.make_async_copy(d_hbm, d_ref, load.at[1]),
        pltpu.make_async_copy(feat_hbm, feat, load.at[2]),
    ]
    for one in loads:
        one.start()
    barrier = pltpu.get_barrier_semaphore()
    partners = [
        to_core, to_yl, to_z_up, to_z_down, to_x_up, to_x_down,
        to_yh, to_z_far, to_x_far, *across,
    ]
    for partner in partners:
        pl.semaphore_signal(barrier, inc=1, device_id=partner, device_id_type=mesh_ids)

    rows, depth = feat.shape
    wide, long = depth // PIECES, rows // PIECES
    started, stores = {}, []

    def lanes(p):
        return pl.ds(p * wide, wide)

    def images(p):
        return pl.ds(p * long, long)

    def push(k, p, number, src, dst, device):
        one = pltpu.make_async_remote_copy(
            src_ref=src,
            dst_ref=dst,
            send_sem=send.at[k, p, number],
            recv_sem=recv.at[k, p, number],
            device_id=device,
            device_id_type=mesh_ids,
        )
        one.start()
        started[k, p, number] = one

    def arrived(k, p, *numbers):
        for number in numbers:
            started[k, p, number].wait_recv()

    def same(k, p, number, ref, device):
        push(k, p, number, ref, ref, device)

    def pack(k):
        both = jnp.concatenate(
            (
                w_ref[...].astype(f32)[8 * k : 8 * k + 8],
                d_ref[...].astype(f32)[8 * k : 8 * k + 8],
            ),
            axis=0,
        )
        gath[k, z, yh, core] = both.astype(bf16)

    def gather_start(k, p):
        if p == 0 and k > 0:
            pack(k)
        mine = gath.at[k, z, yh, core, :, lanes(p)]
        same(k, p, 0, mine, to_yh)
        same(k, p, 1, mine, to_z_up)
        same(k, p, 2, mine, to_z_down)
        same(k, p, 7, mine, to_core)

    def gather_second(k, p):
        arrived(k, p, 0)
        theirs = gath.at[k, z, 1 - yh, core, :, lanes(p)]
        same(k, p, 3, theirs, to_z_up)
        same(k, p, 4, theirs, to_z_down)
        same(k, p, 8, theirs, to_core)

    def gather_forward(k, p):
        arrived(k, p, 1, 3)
        same(k, p, 5, gath.at[k, z_down, 0, core, :, lanes(p)], to_z_up)
        arrived(k, p, 2, 4)
        same(k, p, 6, gath.at[k, z_up, 1, core, :, lanes(p)], to_z_down)
        same(k, p, 9, gath.at[k, z_down, :, core, :, lanes(p)], to_core)
        same(k, p, 10, gath.at[k, z_up, :, core, :, lanes(p)], to_core)

    def gather_last(k, p):
        arrived(k, p, 5)
        same(k, p, 11, gath.at[k, z_far, 0, core, :, lanes(p)], to_core)
        arrived(k, p, 6)
        same(k, p, 12, gath.at[k, z_far, 1, core, :, lanes(p)], to_core)

    def scores(k, _):
        if started.pop("features", None):
            loads[2].wait()
        for p in range(PIECES):
            arrived(k, p, 7, 8, 9, 10, 11, 12)
        for p in range(PIECES):
            both = lax.dot_general(
                gath[k].reshape(-1, depth),
                feat[images(p), :],
                (((1,), (1,)), ((), ())),
                preferred_element_type=f32,
            )
            part[k, :, :, :, images(p)] = both.reshape(YLS, XS, -1, long)
            push(k, p, 13, part.at[k, 0, x_far, :, images(p)], r1.at[k, p, 0], to_x_up)
            push(k, p, 14, part.at[k, 1, x_far, :, images(p)], r1.at[k, p, 1], to_x_down)

    def scores_second(k, p):
        here = images(p)
        arrived(k, p, 13)
        part[k, 0, x_up, :, here] += r1[k, p, 0]
        push(k, p, 15, part.at[k, :, x_up, :, here], r2.at[k, p, 0], to_x_up)
        arrived(k, p, 14)
        part[k, 1, x_down, :, here] += r1[k, p, 1]
        push(k, p, 16, part.at[k, :, x_down, :, here], r2.at[k, p, 1], to_x_down)

    def scores_pair(k, p):
        here = images(p)
        arrived(k, p, 15, 16)
        part[k, 1 - yl, x, :, here] += r2[k, p, 0, 1 - yl] + r2[k, p, 1, 1 - yl]
        push(k, p, 17, part.at[k, 1 - yl, x, :, here], r3.at[k, p], to_yl)
        part[k, yl, x, :, here] += r2[k, p, 0, yl] + r2[k, p, 1, yl]

    def curvature(k, p):
        here = images(p)
        arrived(k, p, 17)
        total = part[k, yl, x, :, here] + r3[k, p]
        pair = total.reshape(2, 2, 8, long)
        prob = jax.nn.sigmoid(pair[:, 0])
        value = prob * (1.0 - prob) * pair[:, 1]
        curv[k, yl, x, :, here] = value.reshape(16, long).astype(bf16)
        mine = curv.at[k, yl, x, :, here]
        for number, device in enumerate((to_yl, to_x_up, to_x_down, *across, to_x_far), 18):
            same(k, p, number, mine, device)

    def terms(k, _):
        for p in range(PIECES):
            arrived(k, p, *range(18, 25))
        tile = 1024
        for p in range(PIECES):

            @pl.loop(0, wide // tile)
            def _(n):
                here = pl.ds(pl.multiple_of(p * wide + n * tile, tile), tile)
                term = jnp.dot(
                    curv[k].reshape(-1, rows), feat[:, here], preferred_element_type=f32
                )
                hess[k, :, :, :, :, here] = term.reshape(ZS, YHS, CORES, 8, tile)

            push(
                k, p, 25, hess.at[k, :, :, 1 - core, :, lanes(p)], r4.at[k, :, :, :, lanes(p)], to_core
            )

    def chip(k, p, place):
        here = lanes(p)
        both = hess[k, place, :, core, :, here] + r4[k, place, :, :, here]
        return both.reshape(16, wide)

    def terms_first(k, p):
        arrived(k, p, 25)
        there = ((26, z_far, to_z_far), (28, z_up, to_z_up), (29, z_down, to_z_down))
        for slot, (number, place, device) in enumerate(there):
            zs[k, p, slot] = chip(k, p, place).astype(bf16)
            push(k, p, number, zs.at[k, p, slot], zr.at[k, p, slot], device)

    def terms_pair(k, p):
        arrived(k, p, 26, 28, 29)
        own = chip(k, p, z)
        for slot in range(3):
            own = own + zr[k, p, slot].astype(f32)
        half = wide // 2
        first = yh == 0
        mine = jnp.where(first, own[:8], own[8:])
        theirs = jnp.where(first, own[8:], own[:8])
        ys[k, p] = jnp.concatenate((theirs[:, :half], theirs[:, half:]), axis=0).astype(bf16)
        push(k, p, 30, ys.at[k, p], yr.at[k, p], to_yh)
        out[k, :, lanes(p)] = mine

    def terms_last(k, p):
        arrived(k, p, 30)
        other = yr[k, p].astype(f32)
        both = jnp.concatenate((other[:8], other[8:]), axis=1)
        out[k, :, lanes(p)] = 4.0 * (out[k, :, lanes(p)] + both)
        there = out_hbm.at[pl.ds(8 * k, 8), lanes(p)]
        one = pltpu.make_async_copy(out.at[k, :, lanes(p)], there, store.at[k, p])
        one.start()
        stores.append(one)

    steps = {one.__name__: one for one in (
        gather_start, gather_second, gather_forward, gather_last, scores, scores_second,
        scores_pair, curvature, terms, terms_first, terms_pair, terms_last,
    )}
    started["features"] = True
    loads[0].wait()
    loads[1].wait()
    pack(0)
    pl.semaphore_wait(barrier, len(partners))
    for place, k, p in ORDER:
        steps[NAMES[place]](k, p)
    for one in started.values():
        one.wait_send()
    for one in stores:
        one.wait()


def body(features, weights, direction):
    rows, depth = features.shape
    mine = weights.shape[0]
    K, Q = CHUNKS, PIECES
    wide, long = depth // Q, rows // Q
    f32, bf16 = jnp.float32, jnp.bfloat16
    vmem = pltpu.VMEM
    return pl.pallas_call(
        kernel,
        out_shape=jax.ShapeDtypeStruct((mine, depth), f32),
        in_specs=[pl.BlockSpec(memory_space=pl.ANY)] * 3,
        out_specs=pl.BlockSpec(memory_space=pl.ANY),
        scratch_shapes=[
            vmem((rows, depth), bf16),
            vmem((mine, depth), bf16),
            vmem((mine, depth), bf16),
            vmem((K, ZS, YHS, CORES, 16, depth), bf16),
            vmem((K, YLS, XS, 32, rows), f32),
            vmem((K, Q, 2, 32, long), f32),
            vmem((K, Q, 2, YLS, 32, long), f32),
            vmem((K, Q, 32, long), f32),
            vmem((K, YLS, XS, 16, rows), bf16),
            vmem((K, ZS, YHS, CORES, 8, depth), f32),
            vmem((K, ZS, YHS, 8, depth), f32),
            vmem((K, Q, 3, 16, wide), bf16),
            vmem((K, Q, 3, 16, wide), bf16),
            vmem((K, Q, 16, wide // 2), bf16),
            vmem((K, Q, 16, wide // 2), bf16),
            vmem((K, 8, depth), f32),
            pltpu.SemaphoreType.DMA((3,)),
            pltpu.SemaphoreType.DMA((K, Q)),
            pltpu.SemaphoreType.DMA((K, Q, COPIES)),
            pltpu.SemaphoreType.DMA((K, Q, COPIES)),
        ],
        compiler_params=pltpu.CompilerParams(
            collective_id=0, has_side_effects=True, vmem_limit_bytes=62 * 2**20
        ),
    )(features, weights, direction)


def solution(mesh):
    placed = (P("img", "feat"), P("img", "feat"), P("img", "feat"))
    return jax.shard_map(
        body, mesh=mesh, in_specs=placed, out_specs=P("img", "feat"), check_vma=False
    )
```

```python
import jax
import jax.numpy as jnp
from jax import lax
from jax.experimental import pallas as pl
from jax.experimental.pallas import tpu as pltpu
from jax.sharding import PartitionSpec as P

ZS, YHS, CORES, YLS, XS = 4, 2, 2, 2, 4
CHUNKS = 4
PIECES = 2
BY_PIECE = {0: 0, 1: 1, 3: 1, 2: 2, 4: 2, 5: 3, 6: 4, 13: 5, 14: 6, 15: 7, 16: 7, 17: 8}
BY_PIECE |= {25: 9, 26: 10, 28: 10, 29: 10, 31: 11}
BY_CHUNK = {7: 0, 8: 0, 9: 0, 10: 0, 11: 0, 12: 0, 18: 1, 21: 1, 22: 1, 23: 1, 19: 2, 20: 3, 24: 4}
SENDS = 64
PAIRED = (2, 3)
NAMES = (
    "gather_start", "gather_second", "gather_forward", "gather_last",
    "scores", "scores_far", "scores_second", "scores_pair", "curvature", "", "",
    "terms", "terms_first", "", "terms_pair",
)
ORDER = (
    (0, 0, 0, 0), (0, 0, 1, 0), (0, 1, 0, 0), (1, 0, 0, 0), (1, 0, 1, 0), (1, 1, 0, 4),
    (2, 0, 0, 4), (2, 0, 1, 4), (0, 1, 1, 0), (2, 1, 0, 3), (3, 0, 0, 3), (1, 1, 1, 3),
    (0, 2, 0, 0), (3, 0, 1, 3), (4, 0, 0, 1), (4, 0, 1, 0), (2, 1, 1, 8), (3, 1, 0, 0),
    (0, 2, 1, 0), (6, 0, 0, 6), (1, 2, 0, 0), (6, 0, 1, 4), (3, 1, 1, 1), (1, 2, 1, 6),
    (4, 1, 0, 0), (2, 2, 0, 3), (7, 0, 0, 0), (4, 1, 1, 0), (2, 2, 1, 0), (0, 3, 0, 0),
    (0, 3, 1, 0), (8, 0, 0, 14), (7, 0, 1, 0), (3, 2, 0, 0), (6, 1, 0, 0), (3, 2, 1, 5),
    (1, 3, 0, 2), (4, 2, 0, 5), (1, 3, 1, 0), (6, 1, 1, 0), (4, 2, 1, 0), (2, 3, 0, 7),
    (5, 2, 0, 16), (8, 0, 1, 0), (2, 3, 1, 0), (5, 2, 1, 3), (3, 3, 0, 6), (7, 1, 1, 5),
    (6, 2, 0, 0), (7, 1, 0, 0), (3, 3, 1, 0), (4, 3, 0, 7), (6, 2, 1, 0), (8, 1, 0, 13),
    (4, 3, 1, 0), (5, 3, 0, 5), (7, 2, 0, 0), (8, 1, 1, 0), (11, 0, 0, 0), (11, 0, 1, 0),
    (5, 3, 1, 6), (6, 3, 0, 3), (12, 0, 0, 0), (7, 2, 1, 0), (6, 3, 1, 5), (8, 2, 0, 0),
    (11, 1, 0, 9), (8, 2, 1, 0), (11, 1, 1, 0), (12, 0, 1, 0), (12, 1, 0, 7), (7, 3, 0, 0),
    (7, 3, 1, 6), (12, 1, 1, 0), (8, 3, 1, 0), (11, 2, 0, 6), (8, 3, 0, 0), (11, 2, 1, 0),
    (14, 1, 0, 0), (14, 0, 0, 0), (14, 0, 1, 0), (12, 2, 0, 17), (12, 2, 1, 3), (11, 3, 0, 1),
    (14, 1, 1, 0), (12, 3, 0, 19), (11, 3, 1, 0), (12, 3, 1, 5), (14, 2, 1, 0), (14, 2, 0, 0),
    (14, 3, 0, 5), (14, 3, 1, 1),
)


def kernel(
    feat_hbm, w_hbm, d_hbm, mine_hbm, theirs_hbm,
    feat, w_ref, d_ref, gath, part, rf, r1, r2, r3, curv, hess, r4,
    zs, zr, ys, out,
    load, store, send, by_piece, by_chunk, last,
):
    f32, bf16 = jnp.float32, jnp.bfloat16
    mesh_ids = pl.DeviceIdType.MESH
    img, col = lax.axis_index("img"), lax.axis_index("feat")
    core = lax.rem(img, CORES)
    yh = lax.rem(img // CORES, YHS)
    z = img // (CORES * YHS)
    x = lax.rem(col, XS)
    yl = col // XS
    z_up, z_down, z_far = lax.rem(z + 1, ZS), lax.rem(z + 3, ZS), lax.rem(z + 2, ZS)
    x_up, x_down, x_far = lax.rem(x + 1, XS), lax.rem(x + 3, XS), lax.rem(x + 2, XS)

    def at(z=z, yh=yh, core=core, yl=yl, x=x):
        return {"img": (z * YHS + yh) * CORES + core, "feat": yl * XS + x}

    to_z_up, to_z_down, to_z_far = at(z=z_up), at(z=z_down), at(z=z_far)
    to_x_up, to_x_down, to_x_far = at(x=x_up), at(x=x_down), at(x=x_far)
    to_yh, to_core, to_yl = at(yh=1 - yh), at(core=1 - core), at(yl=1 - yl)
    across = [at(yl=1 - yl, x=one) for one in (x_up, x_down, x_far)]

    loads = [
        pltpu.make_async_copy(w_hbm, w_ref, load.at[0]),
        pltpu.make_async_copy(d_hbm, d_ref, load.at[1]),
        pltpu.make_async_copy(feat_hbm, feat, load.at[2]),
    ]
    for one in loads:
        one.start()
    barrier = pltpu.get_barrier_semaphore()
    partners = [
        to_core, to_yl, to_z_up, to_z_down, to_x_up, to_x_down,
        to_yh, to_z_far, to_x_far, *across,
    ]
    for partner in partners:
        pl.semaphore_signal(barrier, inc=1, device_id=partner, device_id_type=mesh_ids)

    rows, depth = feat.shape
    wide, long = depth // PIECES, rows // PIECES
    slots, flying, waiting = list(range(SENDS)), [], [loads[2]]

    def lanes(p):
        return pl.ds(p * wide, wide)

    def images(p):
        return pl.ds(p * long, long)

    def receive(k, p, number):
        if number in BY_PIECE:
            return by_piece.at[k, p, BY_PIECE[number]]
        return by_chunk.at[k, BY_CHUNK[number]] if number in BY_CHUNK else last.at[0]

    def retire():
        slot, one = flying.pop(0)
        one.wait_send()
        slots.append(slot)

    def push(k, p, number, src, dst, device):
        if not slots:
            retire()
        slot = slots.pop(0)
        one = pltpu.make_async_remote_copy(
            src_ref=src,
            dst_ref=dst,
            send_sem=send.at[slot],
            recv_sem=receive(k, p, number),
            device_id=device,
            device_id_type=mesh_ids,
        )
        one.start()
        flying.append((slot, one))

    def arrived(k, p, number, ref):
        pltpu.make_async_remote_copy(
            src_ref=ref,
            dst_ref=ref,
            send_sem=send.at[0],
            recv_sem=receive(k, p, number),
            device_id=to_core,
            device_id_type=mesh_ids,
        ).wait_recv()

    def same(k, p, number, ref, device):
        push(k, p, number, ref, ref, device)

    def pack(k):
        both = jnp.concatenate(
            (
                w_ref[...].astype(f32)[8 * k : 8 * k + 8],
                d_ref[...].astype(f32)[8 * k : 8 * k + 8],
            ),
            axis=0,
        )
        gath[k, z, yh, core] = both.astype(bf16)

    def gather_start(k, p):
        if p == 0 and k > 0:
            pack(k)
        mine = gath.at[k, z, yh, core, :, lanes(p)]
        same(k, p, 0, mine, to_yh)
        same(k, p, 1, mine, to_z_up)
        same(k, p, 2, mine, to_z_down)
        same(k, p, 7, mine, to_core)

    def gather_second(k, p):
        theirs = gath.at[k, z, 1 - yh, core, :, lanes(p)]
        arrived(k, p, 0, theirs)
        same(k, p, 3, theirs, to_z_up)
        same(k, p, 4, theirs, to_z_down)
        same(k, p, 8, theirs, to_core)

    def gather_forward(k, p):
        arrived(k, p, 1, gath.at[k, z_down, :, core, :, lanes(p)])
        same(k, p, 5, gath.at[k, z_down, 0, core, :, lanes(p)], to_z_up)
        arrived(k, p, 2, gath.at[k, z_up, :, core, :, lanes(p)])
        same(k, p, 6, gath.at[k, z_up, 1, core, :, lanes(p)], to_z_down)
        same(k, p, 9, gath.at[k, z_down, :, core, :, lanes(p)], to_core)
        same(k, p, 10, gath.at[k, z_up, :, core, :, lanes(p)], to_core)

    def gather_last(k, p):
        arrived(k, p, 5, gath.at[k, z_far, 0, core, :, lanes(p)])
        same(k, p, 11, gath.at[k, z_far, 0, core, :, lanes(p)], to_core)
        arrived(k, p, 6, gath.at[k, z_far, 1, core, :, lanes(p)])
        same(k, p, 12, gath.at[k, z_far, 1, core, :, lanes(p)], to_core)

    def scores(k, p):
        here = images(p)
        if waiting:
            waiting.pop().wait()
        if p == 0:
            arrived(k, p, 7, gath.at[k, :, :, 1 - core])
        both = lax.dot_general(
            gath[k].reshape(-1, depth),
            feat[here, :],
            (((1,), (1,)), ((), ())),
            preferred_element_type=f32,
        )
        part[k, :, :, :, here] = both.reshape(YLS, XS, -1, long)
        if k in PAIRED:
            push(k, p, 31, part.at[k, 1 - yl, x_far, :, here], rf.at[k, p], to_yl)
        else:
            push(k, p, 13, part.at[k, 0, x_far, :, here], r1.at[k, p, 0], to_x_up)
            push(k, p, 14, part.at[k, 1, x_far, :, here], r1.at[k, p, 1], to_x_down)

    def halves(p):
        half = long // 2
        return pl.ds(p * long, half), pl.ds(p * long + half, half), pl.ds(0, half)

    def scores_far(k, p):
        first, second, slot = halves(p)
        arrived(k, p, 31, rf.at[k, p])
        part[k, yl, x_far, :, images(p)] += rf[k, p]
        push(k, p, 13, part.at[k, yl, x_far, :, first], r1.at[k, p, 0, :, slot], to_x_up)
        push(k, p, 14, part.at[k, yl, x_far, :, second], r1.at[k, p, 1, :, slot], to_x_down)

    def scores_second(k, p):
        here = images(p)
        first, second, slot = halves(p)
        up = r1.at[k, p, 0, :, slot] if k in PAIRED else r1.at[k, p, 0]
        down = r1.at[k, p, 1, :, slot] if k in PAIRED else r1.at[k, p, 1]
        arrived(k, p, 13, up)
        if k in PAIRED:
            part[k, yl, x_up, :, first] += r1[k, p, 0, :, slot]
        else:
            part[k, 0, x_up, :, here] += r1[k, p, 0]
        push(k, p, 15, part.at[k, :, x_up, :, here], r2.at[k, p, 0], to_x_up)
        arrived(k, p, 14, down)
        if k in PAIRED:
            part[k, yl, x_down, :, second] += r1[k, p, 1, :, slot]
        else:
            part[k, 1, x_down, :, here] += r1[k, p, 1]
        push(k, p, 16, part.at[k, :, x_down, :, here], r2.at[k, p, 1], to_x_down)

    def scores_pair(k, p):
        here = images(p)
        arrived(k, p, 15, r2.at[k, p])
        part[k, 1 - yl, x, :, here] += r2[k, p, 0, 1 - yl] + r2[k, p, 1, 1 - yl]
        push(k, p, 17, part.at[k, 1 - yl, x, :, here], r3.at[k, p], to_yl)
        part[k, yl, x, :, here] += r2[k, p, 0, yl] + r2[k, p, 1, yl]

    def curvature(k, p):
        here = images(p)
        arrived(k, p, 17, r3.at[k, p])
        total = part[k, yl, x, :, here] + r3[k, p]
        pair = total.reshape(2, 2, 8, long)
        prob = jax.nn.sigmoid(pair[:, 0])
        value = prob * (1.0 - prob) * pair[:, 1]
        curv[k, yl, x, :, here] = value.reshape(16, long).astype(bf16)
        mine = curv.at[k, yl, x, :, here]
        for number, device in enumerate((to_yl, to_x_up, to_x_down, *across, to_x_far), 18):
            same(k, p, number, mine, device)

    def terms(k, p):
        if p == 0:
            arrived(k, p, 18, curv.at[k, 1 - yl])
            for number, place in ((19, x_down), (20, x_up), (24, x_far)):
                arrived(k, p, number, curv.at[k, yl, place])
        tile = 1024

        @pl.loop(0, wide // tile)
        def _(n):
            here = pl.ds(pl.multiple_of(p * wide + n * tile, tile), tile)
            term = jnp.dot(
                curv[k].reshape(-1, rows), feat[:, here], preferred_element_type=f32
            )
            hess[k, :, :, :, :, here] = term.reshape(ZS, YHS, CORES, 8, tile)

        there = lanes(p)
        push(k, p, 25, hess.at[k, :, :, 1 - core, :, there], r4.at[k, :, :, :, there], to_core)

    def chip(k, p, place):
        here = lanes(p)
        both = hess[k, place, :, core, :, here] + r4[k, place, :, :, here]
        return both.reshape(16, wide)

    def terms_first(k, p):
        arrived(k, p, 25, r4.at[k, :, :, :, lanes(p)])
        there = ((26, z_far, to_z_far), (28, z_up, to_z_up), (29, z_down, to_z_down))
        for slot, (number, place, device) in enumerate(there):
            zs[k, p, slot] = chip(k, p, place).astype(bf16)
            push(k, p, number, zs.at[k, p, slot], zr.at[k, p, slot], device)

    def terms_pair(k, p):
        arrived(k, p, 26, zr.at[k, p])
        own = chip(k, p, z)
        for slot in range(3):
            own = own + zr[k, p, slot].astype(f32)
        first = yh == 0
        ys[k, p] = jnp.where(first, own[8:], own[:8]).astype(bf16)
        push(k, p, 30, ys.at[k, p], theirs_hbm.at[k, :, lanes(p)], to_yh)
        out[k, p] = jnp.where(first, own[:8], own[8:])
        pltpu.make_async_copy(out.at[k, p], mine_hbm.at[k, :, lanes(p)], store.at[0]).start()

    steps = {one.__name__: one for one in (
        gather_start, gather_second, gather_forward, gather_last, scores, scores_far,
        scores_second, scores_pair, curvature, terms, terms_first, terms_pair,
    )}
    loads[0].wait()
    loads[1].wait()
    pack(0)
    pl.semaphore_wait(barrier, len(partners))
    for place, k, p, enough in ORDER:
        for _ in range(min(enough, len(flying))):
            retire()
        steps[NAMES[place]](k, p)
    arrived(0, 0, 30, theirs_hbm)
    pltpu.make_async_copy(mine_hbm, mine_hbm, store.at[0]).wait()
    while flying:
        retire()


def body(features, weights, direction):
    rows, depth = features.shape
    mine = weights.shape[0]
    K, Q = CHUNKS, PIECES
    wide, long = depth // Q, rows // Q
    f32, bf16 = jnp.float32, jnp.bfloat16
    vmem = pltpu.VMEM
    own, other = pl.pallas_call(
        kernel,
        out_shape=(
            jax.ShapeDtypeStruct((K, mine // K, depth), f32),
            jax.ShapeDtypeStruct((K, mine // K, depth), bf16),
        ),
        in_specs=[pl.BlockSpec(memory_space=pl.ANY)] * 3,
        out_specs=[pl.BlockSpec(memory_space=pl.ANY)] * 2,
        scratch_shapes=[
            vmem((rows, depth), bf16),
            vmem((mine, depth), bf16),
            vmem((mine, depth), bf16),
            vmem((K, ZS, YHS, CORES, 16, depth), bf16),
            vmem((K, YLS, XS, 32, rows), f32),
            vmem((K, Q, 32, long), f32),
            vmem((K, Q, 2, 32, long), f32),
            vmem((K, Q, 2, YLS, 32, long), f32),
            vmem((K, Q, 32, long), f32),
            vmem((K, YLS, XS, 16, rows), bf16),
            vmem((K, ZS, YHS, CORES, 8, depth), f32),
            vmem((K, ZS, YHS, 8, depth), f32),
            vmem((K, Q, 3, 16, wide), bf16),
            vmem((K, Q, 3, 16, wide), bf16),
            vmem((K, Q, 8, wide), bf16),
            vmem((K, Q, 8, wide), f32),
            pltpu.SemaphoreType.DMA((3,)),
            pltpu.SemaphoreType.DMA((1,)),
            pltpu.SemaphoreType.DMA((SENDS,)),
            pltpu.SemaphoreType.DMA((K, Q, 12)),
            pltpu.SemaphoreType.DMA((K, 5)),
            pltpu.SemaphoreType.DMA((1,)),
        ],
        compiler_params=pltpu.CompilerParams(
            collective_id=0, has_side_effects=True, vmem_limit_bytes=62 * 2**20
        ),
    )(features, weights, direction)
    return (4.0 * (own + other.astype(f32))).reshape(mine, depth)


def solution(mesh):
    placed = (P("img", "feat"), P("img", "feat"), P("img", "feat"))
    return jax.shard_map(
        body, mesh=mesh, in_specs=placed, out_specs=P("img", "feat"), check_vma=False
    )
```

```python
import jax
import jax.numpy as jnp
from jax import lax
from jax.experimental import pallas as pl
from jax.experimental.pallas import tpu as pltpu
from jax.sharding import PartitionSpec as P

ZS, YHS, CORES, YLS, XS = 4, 2, 2, 2, 4
CHUNKS = 4
PIECES = 2
BY_PIECE = {0: 0, 1: 1, 3: 1, 2: 2, 4: 2, 5: 3, 6: 4, 13: 5, 14: 6, 15: 7, 16: 7, 17: 8}
BY_PIECE |= {25: 9, 26: 10, 28: 10, 29: 10, 31: 11}
BY_CHUNK = {7: 0, 8: 0, 9: 0, 10: 0, 11: 0, 12: 0, 18: 1, 21: 1, 22: 1, 23: 1, 19: 2, 20: 3, 24: 4}
BY_CHUNK |= {32: 5}
SENDS = 56
PAIRED = (2, 3)
PAIR_FIRST = (3, 1)
NAMES = (
    "gather_start", "gather_second", "gather_forward", "gather_last",
    "scores", "scores_far", "scores_second", "scores_pair", "curvature", "", "",
    "terms", "terms_first", "terms_second", "terms_pair",
)
ORDER = (
    (0, 0, 0, 0), (0, 0, 1, 0), (0, 1, 1, 0), (1, 0, 0, 0), (1, 0, 1, 0), (1, 1, 1, 4),
    (2, 0, 0, 4), (2, 0, 1, 4), (0, 1, 0, 0), (3, 0, 0, 3), (1, 1, 0, 6), (0, 2, 1, 0),
    (3, 0, 1, 4), (2, 1, 1, 0), (4, 0, 0, 0), (2, 1, 0, 10), (4, 0, 1, 0), (1, 2, 1, 0),
    (0, 2, 0, 0), (6, 0, 0, 4), (1, 2, 0, 5), (3, 1, 1, 0), (0, 3, 0, 0), (6, 0, 1, 0),
    (3, 1, 0, 0), (2, 2, 1, 10), (4, 1, 0, 2), (7, 0, 0, 4), (2, 2, 0, 3), (1, 3, 0, 0),
    (0, 3, 1, 0), (4, 1, 1, 0), (8, 0, 0, 8), (3, 2, 1, 0), (7, 0, 1, 0), (3, 2, 0, 3),
    (6, 1, 0, 0), (1, 3, 1, 0), (4, 2, 0, 11), (6, 1, 1, 0), (2, 3, 0, 0), (4, 2, 1, 0),
    (2, 3, 1, 11), (7, 1, 0, 14), (5, 2, 0, 0), (8, 0, 1, 0), (5, 2, 1, 0), (3, 3, 0, 0),
    (3, 3, 1, 6), (7, 1, 1, 0), (8, 1, 0, 0), (6, 2, 0, 0), (4, 3, 0, 0), (4, 3, 1, 0),
    (8, 1, 1, 0), (11, 0, 0, 0), (5, 3, 0, 28), (6, 2, 1, 0), (7, 2, 0, 7), (11, 0, 1, 0),
    (12, 0, 0, 0), (5, 3, 1, 0), (11, 1, 0, 3), (6, 3, 0, 0), (11, 1, 1, 0), (12, 1, 0, 11),
    (7, 2, 1, 0), (6, 3, 1, 0), (12, 0, 1, 0), (8, 2, 0, 0), (7, 3, 0, 5), (12, 1, 1, 0),
    (8, 2, 1, 0), (7, 3, 1, 5), (14, 1, 0, 0), (8, 3, 0, 0), (8, 3, 1, 7), (11, 2, 0, 0),
    (11, 2, 1, 0), (12, 2, 0, 25), (14, 0, 0, 0), (14, 0, 1, 0), (12, 2, 1, 6), (14, 1, 1, 0),
    (11, 3, 0, 0), (11, 3, 1, 0), (12, 3, 1, 10), (12, 3, 0, 0), (14, 2, 1, 1), (14, 2, 0, 0),
    (13, 3, 1, 5), (14, 3, 0, 5), (14, 3, 1, 3),
)


def kernel(
    feat_hbm, w_hbm, d_hbm, mine_hbm, theirs_hbm,
    feat, w_ref, d_ref, gath, part, rf, r1, r2, r3, curv, hess, r4,
    zs, zr, ys, out, ps, pr, qs, qr,
    load, store, send, by_piece, by_chunk, last,
):
    f32, bf16 = jnp.float32, jnp.bfloat16
    mesh_ids = pl.DeviceIdType.MESH
    img, col = lax.axis_index("img"), lax.axis_index("feat")
    core = lax.rem(img, CORES)
    yh = lax.rem(img // CORES, YHS)
    z = img // (CORES * YHS)
    x = lax.rem(col, XS)
    yl = col // XS
    z_up, z_down, z_far = lax.rem(z + 1, ZS), lax.rem(z + 3, ZS), lax.rem(z + 2, ZS)
    x_up, x_down, x_far = lax.rem(x + 1, XS), lax.rem(x + 3, XS), lax.rem(x + 2, XS)

    def at(z=z, yh=yh, core=core, yl=yl, x=x):
        return {"img": (z * YHS + yh) * CORES + core, "feat": yl * XS + x}

    to_z_up, to_z_down, to_z_far = at(z=z_up), at(z=z_down), at(z=z_far)
    to_x_up, to_x_down, to_x_far = at(x=x_up), at(x=x_down), at(x=x_far)
    to_yh, to_core, to_yl = at(yh=1 - yh), at(core=1 - core), at(yl=1 - yl)
    across = [at(yl=1 - yl, x=one) for one in (x_up, x_down, x_far)]

    loads = [
        pltpu.make_async_copy(w_hbm, w_ref, load.at[0]),
        pltpu.make_async_copy(d_hbm, d_ref, load.at[1]),
        pltpu.make_async_copy(feat_hbm, feat, load.at[2]),
    ]
    for one in loads:
        one.start()
    barrier = pltpu.get_barrier_semaphore()
    partners = [
        to_core, to_yl, to_z_up, to_z_down, to_x_up, to_x_down,
        to_yh, to_z_far, to_x_far, *across,
    ]
    for partner in partners:
        pl.semaphore_signal(barrier, inc=1, device_id=partner, device_id_type=mesh_ids)

    rows, depth = feat.shape
    wide, long = depth // PIECES, rows // PIECES
    slots, flying, waiting = list(range(SENDS)), [], [loads[2]]
    unpacked = list(range(1, CHUNKS))

    def lanes(p):
        return pl.ds(p * wide, wide)

    def images(p):
        return pl.ds(p * long, long)

    def receive(k, p, number):
        if number in BY_PIECE:
            return by_piece.at[k, p, BY_PIECE[number]]
        return by_chunk.at[k, BY_CHUNK[number]] if number in BY_CHUNK else last.at[k]

    def retire():
        slot, one = flying.pop(0)
        one.wait_send()
        slots.append(slot)

    def push(k, p, number, src, dst, device):
        if not slots:
            retire()
        slot = slots.pop(0)
        one = pltpu.make_async_remote_copy(
            src_ref=src,
            dst_ref=dst,
            send_sem=send.at[slot],
            recv_sem=receive(k, p, number),
            device_id=device,
            device_id_type=mesh_ids,
        )
        one.start()
        flying.append((slot, one))

    def arrived(k, p, number, ref):
        pltpu.make_async_remote_copy(
            src_ref=ref,
            dst_ref=ref,
            send_sem=send.at[0],
            recv_sem=receive(k, p, number),
            device_id=to_core,
            device_id_type=mesh_ids,
        ).wait_recv()

    def same(k, p, number, ref, device):
        push(k, p, number, ref, ref, device)

    def pack(k):
        both = jnp.concatenate(
            (
                w_ref[...].astype(f32)[8 * k : 8 * k + 8],
                d_ref[...].astype(f32)[8 * k : 8 * k + 8],
            ),
            axis=0,
        )
        gath[k, z, yh, core] = both.astype(bf16)

    def gather_start(k, p):
        if k in unpacked:
            unpacked.remove(k)
            pack(k)
        mine = gath.at[k, z, yh, core, :, lanes(p)]
        same(k, p, 0, mine, to_yh)
        same(k, p, 1, mine, to_z_up)
        same(k, p, 2, mine, to_z_down)
        same(k, p, 7, mine, to_core)

    def gather_second(k, p):
        theirs = gath.at[k, z, 1 - yh, core, :, lanes(p)]
        arrived(k, p, 0, theirs)
        same(k, p, 3, theirs, to_z_up)
        same(k, p, 4, theirs, to_z_down)
        same(k, p, 8, theirs, to_core)

    def gather_forward(k, p):
        arrived(k, p, 1, gath.at[k, z_down, :, core, :, lanes(p)])
        same(k, p, 5, gath.at[k, z_down, 0, core, :, lanes(p)], to_z_up)
        arrived(k, p, 2, gath.at[k, z_up, :, core, :, lanes(p)])
        same(k, p, 6, gath.at[k, z_up, 1, core, :, lanes(p)], to_z_down)
        same(k, p, 9, gath.at[k, z_down, :, core, :, lanes(p)], to_core)
        same(k, p, 10, gath.at[k, z_up, :, core, :, lanes(p)], to_core)

    def gather_last(k, p):
        arrived(k, p, 5, gath.at[k, z_far, 0, core, :, lanes(p)])
        same(k, p, 11, gath.at[k, z_far, 0, core, :, lanes(p)], to_core)
        arrived(k, p, 6, gath.at[k, z_far, 1, core, :, lanes(p)])
        same(k, p, 12, gath.at[k, z_far, 1, core, :, lanes(p)], to_core)

    def scores(k, p):
        here = images(p)
        if waiting:
            waiting.pop().wait()
        if p == 0:
            arrived(k, p, 7, gath.at[k, :, :, 1 - core])
        both = lax.dot_general(
            gath[k].reshape(-1, depth),
            feat[here, :],
            (((1,), (1,)), ((), ())),
            preferred_element_type=f32,
        )
        part[k, :, :, :, here] = both.reshape(YLS, XS, -1, long)
        if k in PAIRED:
            push(k, p, 31, part.at[k, 1 - yl, x_far, :, here], rf.at[k, p], to_yl)
        else:
            push(k, p, 13, part.at[k, 0, x_far, :, here], r1.at[k, p, 0], to_x_up)
            push(k, p, 14, part.at[k, 1, x_far, :, here], r1.at[k, p, 1], to_x_down)

    def halves(p):
        half = long // 2
        return pl.ds(p * long, half), pl.ds(p * long + half, half), pl.ds(0, half)

    def scores_far(k, p):
        first, second, slot = halves(p)
        arrived(k, p, 31, rf.at[k, p])
        part[k, yl, x_far, :, images(p)] += rf[k, p]
        push(k, p, 13, part.at[k, yl, x_far, :, first], r1.at[k, p, 0, :, slot], to_x_up)
        push(k, p, 14, part.at[k, yl, x_far, :, second], r1.at[k, p, 1, :, slot], to_x_down)

    def scores_second(k, p):
        here = images(p)
        first, second, slot = halves(p)
        up = r1.at[k, p, 0, :, slot] if k in PAIRED else r1.at[k, p, 0]
        down = r1.at[k, p, 1, :, slot] if k in PAIRED else r1.at[k, p, 1]
        arrived(k, p, 13, up)
        if k in PAIRED:
            part[k, yl, x_up, :, first] += r1[k, p, 0, :, slot]
        else:
            part[k, 0, x_up, :, here] += r1[k, p, 0]
        push(k, p, 15, part.at[k, :, x_up, :, here], r2.at[k, p, 0], to_x_up)
        arrived(k, p, 14, down)
        if k in PAIRED:
            part[k, yl, x_down, :, second] += r1[k, p, 1, :, slot]
        else:
            part[k, 1, x_down, :, here] += r1[k, p, 1]
        push(k, p, 16, part.at[k, :, x_down, :, here], r2.at[k, p, 1], to_x_down)

    def scores_pair(k, p):
        here = images(p)
        arrived(k, p, 15, r2.at[k, p])
        part[k, 1 - yl, x, :, here] += r2[k, p, 0, 1 - yl] + r2[k, p, 1, 1 - yl]
        push(k, p, 17, part.at[k, 1 - yl, x, :, here], r3.at[k, p], to_yl)
        part[k, yl, x, :, here] += r2[k, p, 0, yl] + r2[k, p, 1, yl]

    def curvature(k, p):
        here = images(p)
        arrived(k, p, 17, r3.at[k, p])
        total = part[k, yl, x, :, here] + r3[k, p]
        pair = total.reshape(2, 2, 8, long)
        prob = jax.nn.sigmoid(pair[:, 0])
        value = prob * (1.0 - prob) * pair[:, 1]
        curv[k, yl, x, :, here] = value.reshape(16, long).astype(bf16)
        mine = curv.at[k, yl, x, :, here]
        for number, device in enumerate((to_yl, to_x_up, to_x_down, *across, to_x_far), 18):
            same(k, p, number, mine, device)

    def terms(k, p):
        if p == 0:
            arrived(k, p, 18, curv.at[k, 1 - yl])
            for number, place in ((19, x_down), (20, x_up), (24, x_far)):
                arrived(k, p, number, curv.at[k, yl, place])
        tile = 1024

        @pl.loop(0, wide // tile)
        def _(n):
            here = pl.ds(pl.multiple_of(p * wide + n * tile, tile), tile)
            term = jnp.dot(
                curv[k].reshape(-1, rows), feat[:, here], preferred_element_type=f32
            )
            hess[k, :, :, :, :, here] = term.reshape(ZS, YHS, CORES, 8, tile)

        there = lanes(p)
        push(k, p, 25, hess.at[k, :, :, 1 - core, :, there], r4.at[k, :, :, :, there], to_core)

    def chip(k, p, place):
        here = lanes(p)
        both = hess[k, place, :, core, :, here] + r4[k, place, :, :, here]
        return both.reshape(16, wide)

    def part_of(k, p, place, half):
        return hess[k, place, half, core, :, lanes(p)] + r4[k, place, half, :, lanes(p)]

    def terms_first(k, p):
        arrived(k, p, 25, r4.at[k, :, :, :, lanes(p)])
        if (k, p) == PAIR_FIRST:
            for place in range(ZS):
                ps[place] = part_of(k, p, place, 1 - yh).astype(bf16)
            push(k, p, 32, ps, pr, to_yh)
            return
        there = ((26, z_far, to_z_far), (28, z_up, to_z_up), (29, z_down, to_z_down))
        for slot, (number, place, device) in enumerate(there):
            zs[k, p, slot] = chip(k, p, place).astype(bf16)
            push(k, p, number, zs.at[k, p, slot], zr.at[k, p, slot], device)

    def terms_second(k, p):
        arrived(k, p, 32, pr)
        there = (
            (30, z_far, to_z_far, theirs_hbm.at[k, :, lanes(p)]),
            (28, z_up, to_z_up, qr.at[0]),
            (29, z_down, to_z_down, qr.at[1]),
        )
        for slot, (number, place, device, dst) in enumerate(there):
            qs[slot] = (part_of(k, p, place, yh) + pr[place].astype(f32)).astype(bf16)
            push(k, p, number, qs.at[slot], dst, device)

    def keep(k, p, value):
        out[k, p] = value
        pltpu.make_async_copy(out.at[k, p], mine_hbm.at[k, :, lanes(p)], store.at[0]).start()

    def terms_pair(k, p):
        if (k, p) == PAIR_FIRST:
            arrived(k, p, 28, qr)
            own = part_of(k, p, z, yh) + pr[z].astype(f32)
            keep(k, p, own + qr[0].astype(f32) + qr[1].astype(f32))
            return
        arrived(k, p, 26, zr.at[k, p])
        own = chip(k, p, z)
        for slot in range(3):
            own = own + zr[k, p, slot].astype(f32)
        first = yh == 0
        ys[k, p] = jnp.where(first, own[8:], own[:8]).astype(bf16)
        push(k, p, 30, ys.at[k, p], theirs_hbm.at[k, :, lanes(p)], to_yh)
        keep(k, p, jnp.where(first, own[:8], own[8:]))

    steps = {one.__name__: one for one in (
        gather_start, gather_second, gather_forward, gather_last, scores, scores_far,
        scores_second, scores_pair, curvature, terms, terms_first, terms_second, terms_pair,
    )}
    loads[0].wait()
    loads[1].wait()
    pack(0)
    pl.semaphore_wait(barrier, len(partners))
    for place, k, p, enough in ORDER:
        for _ in range(min(enough, len(flying))):
            retire()
        steps[NAMES[place]](k, p)
    for k in range(CHUNKS):
        arrived(k, 0, 30, theirs_hbm.at[k])
    pltpu.make_async_copy(mine_hbm, mine_hbm, store.at[0]).wait()
    while flying:
        retire()


def body(features, weights, direction):
    rows, depth = features.shape
    mine = weights.shape[0]
    K, Q = CHUNKS, PIECES
    wide, long = depth // Q, rows // Q
    f32, bf16 = jnp.float32, jnp.bfloat16
    vmem = pltpu.VMEM
    own, other = pl.pallas_call(
        kernel,
        out_shape=(
            jax.ShapeDtypeStruct((K, mine // K, depth), f32),
            jax.ShapeDtypeStruct((K, mine // K, depth), bf16),
        ),
        in_specs=[pl.BlockSpec(memory_space=pl.ANY)] * 3,
        out_specs=[pl.BlockSpec(memory_space=pl.ANY)] * 2,
        scratch_shapes=[
            vmem((rows, depth), bf16),
            vmem((mine, depth), bf16),
            vmem((mine, depth), bf16),
            vmem((K, ZS, YHS, CORES, 16, depth), bf16),
            vmem((K, YLS, XS, 32, rows), f32),
            vmem((K, Q, 32, long), f32),
            vmem((K, Q, 2, 32, long), f32),
            vmem((K, Q, 2, YLS, 32, long), f32),
            vmem((K, Q, 32, long), f32),
            vmem((K, YLS, XS, 16, rows), bf16),
            vmem((K, ZS, YHS, CORES, 8, depth), f32),
            vmem((K, ZS, YHS, 8, depth), f32),
            vmem((K, Q, 3, 16, wide), bf16),
            vmem((K, Q, 3, 16, wide), bf16),
            vmem((K, Q, 8, wide), bf16),
            vmem((K, Q, 8, wide), f32),
            vmem((ZS, 8, wide), bf16),
            vmem((ZS, 8, wide), bf16),
            vmem((3, 8, wide), bf16),
            vmem((2, 8, wide), bf16),
            pltpu.SemaphoreType.DMA((3,)),
            pltpu.SemaphoreType.DMA((1,)),
            pltpu.SemaphoreType.DMA((SENDS,)),
            pltpu.SemaphoreType.DMA((K, Q, 12)),
            pltpu.SemaphoreType.DMA((K, 6)),
            pltpu.SemaphoreType.DMA((K,)),
        ],
        compiler_params=pltpu.CompilerParams(
            collective_id=0, has_side_effects=True, vmem_limit_bytes=62 * 2**20
        ),
    )(features, weights, direction)
    return (4.0 * (own + other.astype(f32))).reshape(mine, depth)


def solution(mesh):
    placed = (P("img", "feat"), P("img", "feat"), P("img", "feat"))
    return jax.shard_map(
        body, mesh=mesh, in_specs=placed, out_specs=P("img", "feat"), check_vma=False
    )
```

```python
import jax
import jax.numpy as jnp
from jax import lax
from jax.experimental import pallas as pl
from jax.experimental.pallas import tpu as pltpu
from jax.sharding import PartitionSpec as P

ZS, YHS, CORES, YLS, XS = 4, 2, 2, 2, 4
CHUNKS = 4
PIECES = 2
BY_PIECE = {0: 0, 1: 1, 3: 1, 2: 2, 4: 2, 5: 3, 6: 4, 13: 5, 14: 6, 15: 7, 16: 7, 17: 8}
BY_PIECE |= {25: 9, 26: 10, 28: 10, 29: 10, 31: 11}
BY_CHUNK = {7: 0, 8: 0, 9: 0, 10: 0, 11: 0, 12: 0, 18: 1, 21: 1, 22: 1, 23: 1, 19: 2, 20: 3, 24: 4}
BY_CHUNK |= {32: 5}
SENDS = 56
PAIRED = (2, 3)
PAIR_FIRST = (3, 1)
RING_FIRST = (0, 1)
NAMES = (
    "gather_start", "gather_second", "gather_forward", "gather_last",
    "scores", "scores_far", "scores_second", "scores_pair", "curvature", "", "",
    "terms", "terms_first", "terms_second", "terms_pair",
)
ORDER = (
    (0, 0, 1, 0), (0, 0, 0, 0), (0, 1, 0, 0), (1, 0, 1, 0), (1, 0, 0, 0), (0, 1, 1, 0),
    (1, 1, 0, 4), (2, 0, 1, 4), (2, 0, 0, 4), (0, 2, 0, 0), (1, 1, 1, 4), (3, 0, 1, 7),
    (3, 0, 0, 5), (0, 2, 1, 0), (2, 1, 0, 0), (1, 2, 0, 2), (4, 0, 0, 4), (4, 0, 1, 0),
    (2, 1, 1, 0), (1, 2, 1, 0), (6, 0, 0, 11), (0, 3, 0, 0), (2, 2, 0, 4), (3, 1, 1, 4),
    (3, 1, 0, 0), (6, 0, 1, 0), (2, 2, 1, 7), (0, 3, 1, 0), (1, 3, 0, 0), (4, 1, 0, 0),
    (7, 0, 0, 0), (4, 1, 1, 0), (7, 0, 1, 13), (3, 2, 0, 0), (1, 3, 1, 0), (8, 0, 0, 8),
    (3, 2, 1, 0), (6, 1, 0, 2), (4, 2, 0, 0), (2, 3, 0, 0), (4, 2, 1, 0), (6, 1, 1, 0),
    (2, 3, 1, 0), (5, 2, 0, 19), (7, 1, 0, 12), (3, 3, 0, 0), (5, 2, 1, 0), (8, 0, 1, 0),
    (3, 3, 1, 0), (8, 1, 0, 7), (6, 2, 1, 1), (7, 1, 1, 0), (4, 3, 0, 0), (6, 2, 0, 0),
    (4, 3, 1, 0), (11, 0, 0, 0), (5, 3, 0, 29), (8, 1, 1, 0), (5, 3, 1, 0), (6, 3, 0, 1),
    (12, 0, 0, 0), (7, 2, 1, 0), (7, 2, 0, 0), (11, 1, 0, 7), (6, 3, 1, 0), (11, 1, 1, 0),
    (8, 2, 1, 0), (12, 1, 0, 11), (8, 2, 0, 0), (7, 3, 0, 0), (12, 1, 1, 0), (11, 0, 1, 0),
    (7, 3, 1, 8), (12, 0, 1, 0), (8, 3, 0, 0), (8, 3, 1, 7), (11, 2, 0, 0), (11, 2, 1, 0),
    (14, 0, 0, 0), (12, 2, 0, 19), (11, 3, 0, 0), (11, 3, 1, 0), (14, 0, 1, 0), (14, 1, 1, 0),
    (12, 2, 1, 0), (12, 3, 1, 20), (14, 1, 0, 0), (14, 2, 0, 1), (12, 3, 0, 0), (13, 3, 1, 0),
    (14, 2, 1, 0), (14, 3, 0, 9), (14, 3, 1, 2),
)


def kernel(
    feat_hbm, w_hbm, d_hbm, mine_hbm, theirs_hbm,
    feat, w_ref, d_ref, gath, part, rf, r1, r2, r3, curv, hess, r4,
    zs, zr, ys, out, ps, pr, qs, qr,
    load, store, send, by_piece, by_chunk, last,
):
    f32, bf16 = jnp.float32, jnp.bfloat16
    mesh_ids = pl.DeviceIdType.MESH
    img, col = lax.axis_index("img"), lax.axis_index("feat")
    core = lax.rem(img, CORES)
    yh = lax.rem(img // CORES, YHS)
    z = img // (CORES * YHS)
    x = lax.rem(col, XS)
    yl = col // XS
    z_up, z_down, z_far = lax.rem(z + 1, ZS), lax.rem(z + 3, ZS), lax.rem(z + 2, ZS)
    x_up, x_down, x_far = lax.rem(x + 1, XS), lax.rem(x + 3, XS), lax.rem(x + 2, XS)

    def at(z=z, yh=yh, core=core, yl=yl, x=x):
        return {"img": (z * YHS + yh) * CORES + core, "feat": yl * XS + x}

    to_z_up, to_z_down, to_z_far = at(z=z_up), at(z=z_down), at(z=z_far)
    to_x_up, to_x_down, to_x_far = at(x=x_up), at(x=x_down), at(x=x_far)
    to_yh, to_core, to_yl = at(yh=1 - yh), at(core=1 - core), at(yl=1 - yl)
    across = [at(yl=1 - yl, x=one) for one in (x_up, x_down, x_far)]

    loads = [
        pltpu.make_async_copy(w_hbm, w_ref, load.at[0]),
        pltpu.make_async_copy(d_hbm, d_ref, load.at[1]),
        pltpu.make_async_copy(feat_hbm, feat, load.at[2]),
    ]
    for one in loads:
        one.start()
    barrier = pltpu.get_barrier_semaphore()
    partners = [
        to_core, to_yl, to_z_up, to_z_down, to_x_up, to_x_down,
        to_yh, to_z_far, to_x_far, *across,
    ]
    for partner in partners:
        pl.semaphore_signal(barrier, inc=1, device_id=partner, device_id_type=mesh_ids)

    rows, depth = feat.shape
    wide, long = depth // PIECES, rows // PIECES
    slots, flying, waiting = list(range(SENDS)), [], [loads[2]]
    unpacked = list(range(1, CHUNKS))

    def lanes(p):
        return pl.ds(p * wide, wide)

    def images(p):
        return pl.ds(p * long, long)

    def receive(k, p, number):
        if number in BY_PIECE:
            return by_piece.at[k, p, BY_PIECE[number]]
        return by_chunk.at[k, BY_CHUNK[number]] if number in BY_CHUNK else last.at[k]

    def retire():
        slot, one = flying.pop(0)
        one.wait_send()
        slots.append(slot)

    def push(k, p, number, src, dst, device):
        if not slots:
            retire()
        slot = slots.pop(0)
        one = pltpu.make_async_remote_copy(
            src_ref=src,
            dst_ref=dst,
            send_sem=send.at[slot],
            recv_sem=receive(k, p, number),
            device_id=device,
            device_id_type=mesh_ids,
        )
        one.start()
        flying.append((slot, one))

    def arrived(k, p, number, ref):
        pltpu.make_async_remote_copy(
            src_ref=ref,
            dst_ref=ref,
            send_sem=send.at[0],
            recv_sem=receive(k, p, number),
            device_id=to_core,
            device_id_type=mesh_ids,
        ).wait_recv()

    def same(k, p, number, ref, device):
        push(k, p, number, ref, ref, device)

    def pack(k):
        both = jnp.concatenate(
            (
                w_ref[...].astype(f32)[8 * k : 8 * k + 8],
                d_ref[...].astype(f32)[8 * k : 8 * k + 8],
            ),
            axis=0,
        )
        gath[k, z, yh, core] = both.astype(bf16)

    def gather_start(k, p):
        if k in unpacked:
            unpacked.remove(k)
            pack(k)
        mine = gath.at[k, z, yh, core, :, lanes(p)]
        same(k, p, 1, mine, to_z_up)
        same(k, p, 2, mine, to_z_down)
        same(k, p, 0, mine, to_yh)
        same(k, p, 7, mine, to_core)

    def ring_second(k, p):
        half = wide // 2
        down = gath.at[k, z_down, yh, core]
        arrived(k, p, 1, down.at[:, lanes(p)])
        same(k, p, 5, down.at[:, pl.ds(p * wide, half)], to_z_up)
        same(k, p, 0, down.at[:, lanes(p)], to_yh)
        same(k, p, 9, down.at[:, lanes(p)], to_core)
        up = gath.at[k, z_up, yh, core]
        arrived(k, p, 2, up.at[:, lanes(p)])
        same(k, p, 6, up.at[:, pl.ds(p * wide + half, half)], to_z_down)
        same(k, p, 0, up.at[:, lanes(p)], to_yh)
        same(k, p, 10, up.at[:, lanes(p)], to_core)

    def ring_forward(k, p):
        half = wide // 2
        far = gath.at[k, z_far, yh, core]
        arrived(k, p, 5, far.at[:, pl.ds(p * wide, half)])
        arrived(k, p, 6, far.at[:, pl.ds(p * wide + half, half)])
        same(k, p, 0, far.at[:, lanes(p)], to_yh)
        same(k, p, 11, far.at[:, lanes(p)], to_core)

    def ring_last(k, p):
        theirs = gath.at[k, :, 1 - yh, core, :, lanes(p)]
        arrived(k, p, 0, theirs)
        same(k, p, 12, theirs, to_core)

    def gather_second(k, p):
        if (k, p) == RING_FIRST:
            return ring_second(k, p)
        theirs = gath.at[k, z, 1 - yh, core, :, lanes(p)]
        arrived(k, p, 0, theirs)
        same(k, p, 3, theirs, to_z_up)
        same(k, p, 4, theirs, to_z_down)
        same(k, p, 8, theirs, to_core)

    def gather_forward(k, p):
        if (k, p) == RING_FIRST:
            return ring_forward(k, p)
        arrived(k, p, 1, gath.at[k, z_down, :, core, :, lanes(p)])
        same(k, p, 5, gath.at[k, z_down, 0, core, :, lanes(p)], to_z_up)
        arrived(k, p, 2, gath.at[k, z_up, :, core, :, lanes(p)])
        same(k, p, 6, gath.at[k, z_up, 1, core, :, lanes(p)], to_z_down)
        same(k, p, 9, gath.at[k, z_down, :, core, :, lanes(p)], to_core)
        same(k, p, 10, gath.at[k, z_up, :, core, :, lanes(p)], to_core)

    def gather_last(k, p):
        if (k, p) == RING_FIRST:
            return ring_last(k, p)
        arrived(k, p, 5, gath.at[k, z_far, 0, core, :, lanes(p)])
        same(k, p, 11, gath.at[k, z_far, 0, core, :, lanes(p)], to_core)
        arrived(k, p, 6, gath.at[k, z_far, 1, core, :, lanes(p)])
        same(k, p, 12, gath.at[k, z_far, 1, core, :, lanes(p)], to_core)

    def scores(k, p):
        here = images(p)
        if waiting:
            waiting.pop().wait()
        if p == 0:
            arrived(k, p, 7, gath.at[k, :, :, 1 - core])
        both = lax.dot_general(
            gath[k].reshape(-1, depth),
            feat[here, :],
            (((1,), (1,)), ((), ())),
            preferred_element_type=f32,
        )
        part[k, :, :, :, here] = both.reshape(YLS, XS, -1, long)
        if k in PAIRED:
            push(k, p, 31, part.at[k, 1 - yl, x_far, :, here], rf.at[k, p], to_yl)
        else:
            push(k, p, 13, part.at[k, 0, x_far, :, here], r1.at[k, p, 0], to_x_up)
            push(k, p, 14, part.at[k, 1, x_far, :, here], r1.at[k, p, 1], to_x_down)

    def halves(p):
        half = long // 2
        return pl.ds(p * long, half), pl.ds(p * long + half, half), pl.ds(0, half)

    def scores_far(k, p):
        first, second, slot = halves(p)
        arrived(k, p, 31, rf.at[k, p])
        part[k, yl, x_far, :, images(p)] += rf[k, p]
        push(k, p, 13, part.at[k, yl, x_far, :, first], r1.at[k, p, 0, :, slot], to_x_up)
        push(k, p, 14, part.at[k, yl, x_far, :, second], r1.at[k, p, 1, :, slot], to_x_down)

    def scores_second(k, p):
        here = images(p)
        first, second, slot = halves(p)
        up = r1.at[k, p, 0, :, slot] if k in PAIRED else r1.at[k, p, 0]
        down = r1.at[k, p, 1, :, slot] if k in PAIRED else r1.at[k, p, 1]
        arrived(k, p, 13, up)
        if k in PAIRED:
            part[k, yl, x_up, :, first] += r1[k, p, 0, :, slot]
        else:
            part[k, 0, x_up, :, here] += r1[k, p, 0]
        push(k, p, 15, part.at[k, :, x_up, :, here], r2.at[k, p, 0], to_x_up)
        arrived(k, p, 14, down)
        if k in PAIRED:
            part[k, yl, x_down, :, second] += r1[k, p, 1, :, slot]
        else:
            part[k, 1, x_down, :, here] += r1[k, p, 1]
        push(k, p, 16, part.at[k, :, x_down, :, here], r2.at[k, p, 1], to_x_down)

    def scores_pair(k, p):
        here = images(p)
        arrived(k, p, 15, r2.at[k, p])
        part[k, 1 - yl, x, :, here] += r2[k, p, 0, 1 - yl] + r2[k, p, 1, 1 - yl]
        push(k, p, 17, part.at[k, 1 - yl, x, :, here], r3.at[k, p], to_yl)
        part[k, yl, x, :, here] += r2[k, p, 0, yl] + r2[k, p, 1, yl]

    def curvature(k, p):
        here = images(p)
        arrived(k, p, 17, r3.at[k, p])
        total = part[k, yl, x, :, here] + r3[k, p]
        pair = total.reshape(2, 2, 8, long)
        prob = jax.nn.sigmoid(pair[:, 0])
        value = prob * (1.0 - prob) * pair[:, 1]
        curv[k, yl, x, :, here] = value.reshape(16, long).astype(bf16)
        mine = curv.at[k, yl, x, :, here]
        for number, device in enumerate((to_yl, to_x_up, to_x_down, *across, to_x_far), 18):
            same(k, p, number, mine, device)

    def terms(k, p):
        if p == 0:
            arrived(k, p, 18, curv.at[k, 1 - yl])
            for number, place in ((19, x_down), (20, x_up), (24, x_far)):
                arrived(k, p, number, curv.at[k, yl, place])
        tile = 1024

        @pl.loop(0, wide // tile)
        def _(n):
            here = pl.ds(pl.multiple_of(p * wide + n * tile, tile), tile)
            term = jnp.dot(
                curv[k].reshape(-1, rows), feat[:, here], preferred_element_type=f32
            )
            hess[k, :, :, :, :, here] = term.reshape(ZS, YHS, CORES, 8, tile)

        there = lanes(p)
        push(k, p, 25, hess.at[k, :, :, 1 - core, :, there], r4.at[k, :, :, :, there], to_core)

    def chip(k, p, place):
        here = lanes(p)
        both = hess[k, place, :, core, :, here] + r4[k, place, :, :, here]
        return both.reshape(16, wide)

    def part_of(k, p, place, half):
        return hess[k, place, half, core, :, lanes(p)] + r4[k, place, half, :, lanes(p)]

    def terms_first(k, p):
        arrived(k, p, 25, r4.at[k, :, :, :, lanes(p)])
        if (k, p) == PAIR_FIRST:
            for place in range(ZS):
                ps[place] = part_of(k, p, place, 1 - yh).astype(bf16)
            push(k, p, 32, ps, pr, to_yh)
            return
        there = ((26, z_far, to_z_far), (28, z_up, to_z_up), (29, z_down, to_z_down))
        for slot, (number, place, device) in enumerate(there):
            zs[k, p, slot] = chip(k, p, place).astype(bf16)
            push(k, p, number, zs.at[k, p, slot], zr.at[k, p, slot], device)

    def terms_second(k, p):
        arrived(k, p, 32, pr)
        there = (
            (30, z_far, to_z_far, theirs_hbm.at[k, :, lanes(p)]),
            (28, z_up, to_z_up, qr.at[0]),
            (29, z_down, to_z_down, qr.at[1]),
        )
        for slot, (number, place, device, dst) in enumerate(there):
            qs[slot] = (part_of(k, p, place, yh) + pr[place].astype(f32)).astype(bf16)
            push(k, p, number, qs.at[slot], dst, device)

    def keep(k, p, value):
        out[k, p] = value
        pltpu.make_async_copy(out.at[k, p], mine_hbm.at[k, :, lanes(p)], store.at[0]).start()

    def terms_pair(k, p):
        if (k, p) == PAIR_FIRST:
            arrived(k, p, 28, qr)
            own = part_of(k, p, z, yh) + pr[z].astype(f32)
            keep(k, p, own + qr[0].astype(f32) + qr[1].astype(f32))
            return
        arrived(k, p, 26, zr.at[k, p])
        own = chip(k, p, z)
        for slot in range(3):
            own = own + zr[k, p, slot].astype(f32)
        first = yh == 0
        ys[k, p] = jnp.where(first, own[8:], own[:8]).astype(bf16)
        push(k, p, 30, ys.at[k, p], theirs_hbm.at[k, :, lanes(p)], to_yh)
        keep(k, p, jnp.where(first, own[:8], own[8:]))

    steps = {one.__name__: one for one in (
        gather_start, gather_second, gather_forward, gather_last, scores, scores_far,
        scores_second, scores_pair, curvature, terms, terms_first, terms_second, terms_pair,
    )}
    loads[0].wait()
    loads[1].wait()
    pack(0)
    pl.semaphore_wait(barrier, len(partners))
    for place, k, p, enough in ORDER:
        for _ in range(min(enough, len(flying))):
            retire()
        steps[NAMES[place]](k, p)
    for k in range(CHUNKS):
        arrived(k, 0, 30, theirs_hbm.at[k])
    pltpu.make_async_copy(mine_hbm, mine_hbm, store.at[0]).wait()
    while flying:
        retire()


def body(features, weights, direction):
    rows, depth = features.shape
    mine = weights.shape[0]
    K, Q = CHUNKS, PIECES
    wide, long = depth // Q, rows // Q
    f32, bf16 = jnp.float32, jnp.bfloat16
    vmem = pltpu.VMEM
    own, other = pl.pallas_call(
        kernel,
        out_shape=(
            jax.ShapeDtypeStruct((K, mine // K, depth), f32),
            jax.ShapeDtypeStruct((K, mine // K, depth), bf16),
        ),
        in_specs=[pl.BlockSpec(memory_space=pl.ANY)] * 3,
        out_specs=[pl.BlockSpec(memory_space=pl.ANY)] * 2,
        scratch_shapes=[
            vmem((rows, depth), bf16),
            vmem((mine, depth), bf16),
            vmem((mine, depth), bf16),
            vmem((K, ZS, YHS, CORES, 16, depth), bf16),
            vmem((K, YLS, XS, 32, rows), f32),
            vmem((K, Q, 32, long), f32),
            vmem((K, Q, 2, 32, long), f32),
            vmem((K, Q, 2, YLS, 32, long), f32),
            vmem((K, Q, 32, long), f32),
            vmem((K, YLS, XS, 16, rows), bf16),
            vmem((K, ZS, YHS, CORES, 8, depth), f32),
            vmem((K, ZS, YHS, 8, depth), f32),
            vmem((K, Q, 3, 16, wide), bf16),
            vmem((K, Q, 3, 16, wide), bf16),
            vmem((K, Q, 8, wide), bf16),
            vmem((K, Q, 8, wide), f32),
            vmem((ZS, 8, wide), bf16),
            vmem((ZS, 8, wide), bf16),
            vmem((3, 8, wide), bf16),
            vmem((2, 8, wide), bf16),
            pltpu.SemaphoreType.DMA((3,)),
            pltpu.SemaphoreType.DMA((1,)),
            pltpu.SemaphoreType.DMA((SENDS,)),
            pltpu.SemaphoreType.DMA((K, Q, 12)),
            pltpu.SemaphoreType.DMA((K, 6)),
            pltpu.SemaphoreType.DMA((K,)),
        ],
        compiler_params=pltpu.CompilerParams(
            collective_id=0, has_side_effects=True, vmem_limit_bytes=62 * 2**20
        ),
    )(features, weights, direction)
    return (4.0 * (own + other.astype(f32))).reshape(mine, depth)


def solution(mesh):
    placed = (P("img", "feat"), P("img", "feat"), P("img", "feat"))
    return jax.shard_map(
        body, mesh=mesh, in_specs=placed, out_specs=P("img", "feat"), check_vma=False
    )
```

```python
import jax
import jax.numpy as jnp
from jax import lax
from jax.experimental import pallas as pl
from jax.experimental.pallas import tpu as pltpu
from jax.sharding import PartitionSpec as P

ZS, YHS, CORES, YLS, XS = 4, 2, 2, 2, 4
CHUNKS = 4
PIECES = 2
BY_PIECE = {0: 0, 1: 1, 3: 1, 2: 2, 4: 2, 5: 3, 6: 4, 13: 5, 14: 6, 15: 7, 16: 7, 17: 8}
BY_PIECE |= {25: 9, 26: 10, 28: 10, 29: 10, 31: 11}
BY_CHUNK = {7: 0, 8: 0, 9: 0, 10: 0, 11: 0, 12: 0, 18: 1, 21: 1, 22: 1, 23: 1, 19: 2, 20: 3, 24: 4}
BY_CHUNK |= {32: 5}
SENDS = 48
PAIRED = (2, 3)
PAIR_FIRST = (3, 1)
RING_FIRST = (0, 1)
NAMES = (
    "gather_start", "gather_second", "gather_forward", "gather_last",
    "scores", "scores_far", "scores_second", "scores_pair", "curvature", "", "",
    "terms", "terms_first", "terms_second", "terms_pair",
)
ORDER = (
    (0, 0, 1, 0), (0, 0, 0, 0), (0, 1, 1, 0), (1, 0, 1, 0), (1, 0, 0, 0), (0, 1, 0, 0),
    (1, 1, 1, 4), (2, 0, 1, 4), (2, 0, 0, 4), (1, 1, 0, 4), (3, 0, 1, 7), (2, 1, 1, 0),
    (3, 0, 0, 5), (0, 2, 1, 0), (4, 0, 0, 2), (2, 1, 0, 0), (0, 2, 0, 0), (4, 0, 1, 0),
    (1, 2, 1, 0), (3, 1, 1, 0), (1, 2, 0, 15), (6, 0, 0, 0), (3, 1, 0, 0), (0, 3, 0, 0),
    (4, 1, 0, 4), (2, 2, 1, 3), (4, 1, 1, 0), (2, 2, 0, 0), (6, 0, 1, 0), (0, 3, 1, 0),
    (3, 2, 1, 14), (1, 3, 0, 0), (7, 0, 0, 0), (6, 1, 0, 0), (6, 1, 1, 10), (3, 2, 0, 7),
    (1, 3, 1, 0), (4, 2, 0, 2), (2, 3, 0, 4), (7, 0, 1, 0), (4, 2, 1, 0), (2, 3, 1, 0),
    (5, 2, 0, 12), (8, 0, 0, 0), (3, 3, 0, 1), (8, 0, 1, 1), (5, 2, 1, 0), (3, 3, 1, 0),
    (6, 2, 0, 0), (7, 1, 0, 0), (4, 3, 0, 13), (4, 3, 1, 0), (6, 2, 1, 0), (7, 1, 1, 0),
    (11, 0, 0, 0), (5, 3, 0, 25), (8, 1, 0, 0), (12, 0, 0, 2), (5, 3, 1, 0), (8, 1, 1, 0),
    (11, 0, 1, 0), (6, 3, 0, 5), (7, 2, 1, 0), (12, 0, 1, 4), (7, 2, 0, 0), (6, 3, 1, 5),
    (8, 2, 1, 5), (11, 1, 0, 0), (11, 1, 1, 0), (8, 2, 0, 0), (12, 1, 1, 12), (7, 3, 0, 0),
    (7, 3, 1, 7), (12, 1, 0, 0), (8, 3, 0, 0), (8, 3, 1, 5), (11, 2, 0, 0), (14, 1, 1, 0),
    (11, 2, 1, 0), (12, 2, 0, 19), (14, 0, 1, 0), (11, 3, 0, 0), (11, 3, 1, 0), (12, 2, 1, 0),
    (14, 1, 0, 0), (12, 3, 1, 18), (14, 0, 0, 0), (12, 3, 0, 0), (14, 2, 1, 0), (14, 2, 0, 0),
    (13, 3, 1, 6), (14, 3, 0, 3), (14, 3, 1, 3),
)


def kernel(
    feat_hbm, w_hbm, d_hbm, mine_hbm, theirs_hbm,
    feat, w_ref, d_ref, gath, part, rf, r1, r2, r3, curv, hess, r4,
    zs, zr, ys, out, ps, pr, qs, qr,
    load, store, send, by_piece, by_chunk, last,
):
    f32, bf16 = jnp.float32, jnp.bfloat16
    mesh_ids = pl.DeviceIdType.MESH
    img, col = lax.axis_index("img"), lax.axis_index("feat")
    core = lax.rem(img, CORES)
    yh = lax.rem(img // CORES, YHS)
    z = img // (CORES * YHS)
    x = lax.rem(col, XS)
    yl = col // XS
    z_up, z_down, z_far = lax.rem(z + 1, ZS), lax.rem(z + 3, ZS), lax.rem(z + 2, ZS)
    x_up, x_down, x_far = lax.rem(x + 1, XS), lax.rem(x + 3, XS), lax.rem(x + 2, XS)

    def at(z=z, yh=yh, core=core, yl=yl, x=x):
        return {"img": (z * YHS + yh) * CORES + core, "feat": yl * XS + x}

    to_z_up, to_z_down, to_z_far = at(z=z_up), at(z=z_down), at(z=z_far)
    to_x_up, to_x_down, to_x_far = at(x=x_up), at(x=x_down), at(x=x_far)
    to_yh, to_core, to_yl = at(yh=1 - yh), at(core=1 - core), at(yl=1 - yl)
    across = [at(yl=1 - yl, x=one) for one in (x_up, x_down, x_far)]

    loads = [
        pltpu.make_async_copy(w_hbm, w_ref, load.at[0]),
        pltpu.make_async_copy(d_hbm, d_ref, load.at[1]),
        pltpu.make_async_copy(feat_hbm, feat, load.at[2]),
    ]
    for one in loads:
        one.start()
    barrier = pltpu.get_barrier_semaphore()
    partners = [
        to_core, to_yl, to_z_up, to_z_down, to_x_up, to_x_down,
        to_yh,
    ]
    for partner in partners:
        pl.semaphore_signal(barrier, inc=1, device_id=partner, device_id_type=mesh_ids)

    rows, depth = feat.shape
    wide, long = depth // PIECES, rows // PIECES
    slots, flying, waiting = list(range(SENDS)), [], [loads[2]]
    unpacked = list(range(1, CHUNKS))

    def lanes(p):
        return pl.ds(p * wide, wide)

    def images(p):
        return pl.ds(p * long, long)

    def receive(k, p, number):
        if number in BY_PIECE:
            return by_piece.at[k, p, BY_PIECE[number]]
        return by_chunk.at[k, BY_CHUNK[number]] if number in BY_CHUNK else last.at[k]

    def retire():
        slot, one = flying.pop(0)
        one.wait_send()
        slots.append(slot)

    def push(k, p, number, src, dst, device):
        if not slots:
            retire()
        slot = slots.pop(0)
        one = pltpu.make_async_remote_copy(
            src_ref=src,
            dst_ref=dst,
            send_sem=send.at[slot],
            recv_sem=receive(k, p, number),
            device_id=device,
            device_id_type=mesh_ids,
        )
        one.start()
        flying.append((slot, one))

    def arrived(k, p, number, ref):
        pltpu.make_async_remote_copy(
            src_ref=ref,
            dst_ref=ref,
            send_sem=send.at[0],
            recv_sem=receive(k, p, number),
            device_id=to_core,
            device_id_type=mesh_ids,
        ).wait_recv()

    def same(k, p, number, ref, device):
        push(k, p, number, ref, ref, device)

    def pack(k):
        both = jnp.concatenate(
            (
                w_ref[...].astype(f32)[8 * k : 8 * k + 8],
                d_ref[...].astype(f32)[8 * k : 8 * k + 8],
            ),
            axis=0,
        )
        gath[k, z, yh, core] = both.astype(bf16)

    def gather_start(k, p):
        if k in unpacked:
            unpacked.remove(k)
            pack(k)
        mine = gath.at[k, z, yh, core, :, lanes(p)]
        same(k, p, 1, mine, to_z_up)
        same(k, p, 2, mine, to_z_down)
        same(k, p, 0, mine, to_yh)
        same(k, p, 7, mine, to_core)

    def ring_second(k, p):
        half = wide // 2
        down = gath.at[k, z_down, yh, core]
        arrived(k, p, 1, down.at[:, lanes(p)])
        same(k, p, 5, down.at[:, pl.ds(p * wide, half)], to_z_up)
        same(k, p, 0, down.at[:, lanes(p)], to_yh)
        same(k, p, 9, down.at[:, lanes(p)], to_core)
        up = gath.at[k, z_up, yh, core]
        arrived(k, p, 2, up.at[:, lanes(p)])
        same(k, p, 6, up.at[:, pl.ds(p * wide + half, half)], to_z_down)
        same(k, p, 0, up.at[:, lanes(p)], to_yh)
        same(k, p, 10, up.at[:, lanes(p)], to_core)

    def ring_forward(k, p):
        half = wide // 2
        far = gath.at[k, z_far, yh, core]
        arrived(k, p, 5, far.at[:, pl.ds(p * wide, half)])
        arrived(k, p, 6, far.at[:, pl.ds(p * wide + half, half)])
        same(k, p, 0, far.at[:, lanes(p)], to_yh)
        same(k, p, 11, far.at[:, lanes(p)], to_core)

    def ring_last(k, p):
        theirs = gath.at[k, :, 1 - yh, core, :, lanes(p)]
        arrived(k, p, 0, theirs)
        same(k, p, 12, theirs, to_core)

    def gather_second(k, p):
        if (k, p) == RING_FIRST:
            return ring_second(k, p)
        theirs = gath.at[k, z, 1 - yh, core, :, lanes(p)]
        arrived(k, p, 0, theirs)
        same(k, p, 3, theirs, to_z_up)
        same(k, p, 4, theirs, to_z_down)
        same(k, p, 8, theirs, to_core)

    def gather_forward(k, p):
        if (k, p) == RING_FIRST:
            return ring_forward(k, p)
        arrived(k, p, 1, gath.at[k, z_down, :, core, :, lanes(p)])
        same(k, p, 5, gath.at[k, z_down, 0, core, :, lanes(p)], to_z_up)
        arrived(k, p, 2, gath.at[k, z_up, :, core, :, lanes(p)])
        same(k, p, 6, gath.at[k, z_up, 1, core, :, lanes(p)], to_z_down)
        same(k, p, 9, gath.at[k, z_down, :, core, :, lanes(p)], to_core)
        same(k, p, 10, gath.at[k, z_up, :, core, :, lanes(p)], to_core)

    def gather_last(k, p):
        if (k, p) == RING_FIRST:
            return ring_last(k, p)
        arrived(k, p, 5, gath.at[k, z_far, 0, core, :, lanes(p)])
        same(k, p, 11, gath.at[k, z_far, 0, core, :, lanes(p)], to_core)
        arrived(k, p, 6, gath.at[k, z_far, 1, core, :, lanes(p)])
        same(k, p, 12, gath.at[k, z_far, 1, core, :, lanes(p)], to_core)

    def scores(k, p):
        here = images(p)
        if waiting:
            waiting.pop().wait()
        if p == 0:
            arrived(k, p, 7, gath.at[k, :, :, 1 - core])
        both = lax.dot_general(
            gath[k].reshape(-1, depth),
            feat[here, :],
            (((1,), (1,)), ((), ())),
            preferred_element_type=f32,
        )
        part[k, :, :, :, here] = both.reshape(YLS, XS, -1, long)
        if k in PAIRED:
            push(k, p, 31, part.at[k, 1 - yl, x_far, :, here], rf.at[k, p], to_yl)
        else:
            push(k, p, 13, part.at[k, 0, x_far, :, here], r1.at[k, p, 0], to_x_up)
            push(k, p, 14, part.at[k, 1, x_far, :, here], r1.at[k, p, 1], to_x_down)

    def halves(p):
        half = long // 2
        return pl.ds(p * long, half), pl.ds(p * long + half, half), pl.ds(0, half)

    def scores_far(k, p):
        first, second, slot = halves(p)
        arrived(k, p, 31, rf.at[k, p])
        part[k, yl, x_far, :, images(p)] += rf[k, p]
        push(k, p, 13, part.at[k, yl, x_far, :, first], r1.at[k, p, 0, :, slot], to_x_up)
        push(k, p, 14, part.at[k, yl, x_far, :, second], r1.at[k, p, 1, :, slot], to_x_down)

    def scores_second(k, p):
        here = images(p)
        first, second, slot = halves(p)
        up = r1.at[k, p, 0, :, slot] if k in PAIRED else r1.at[k, p, 0]
        down = r1.at[k, p, 1, :, slot] if k in PAIRED else r1.at[k, p, 1]
        arrived(k, p, 13, up)
        if k in PAIRED:
            part[k, yl, x_up, :, first] += r1[k, p, 0, :, slot]
        else:
            part[k, 0, x_up, :, here] += r1[k, p, 0]
        push(k, p, 15, part.at[k, :, x_up, :, here], r2.at[k, p, 0], to_x_up)
        arrived(k, p, 14, down)
        if k in PAIRED:
            part[k, yl, x_down, :, second] += r1[k, p, 1, :, slot]
        else:
            part[k, 1, x_down, :, here] += r1[k, p, 1]
        push(k, p, 16, part.at[k, :, x_down, :, here], r2.at[k, p, 1], to_x_down)

    def scores_pair(k, p):
        here = images(p)
        arrived(k, p, 15, r2.at[k, p])
        part[k, 1 - yl, x, :, here] += r2[k, p, 0, 1 - yl] + r2[k, p, 1, 1 - yl]
        push(k, p, 17, part.at[k, 1 - yl, x, :, here], r3.at[k, p], to_yl)
        part[k, yl, x, :, here] += r2[k, p, 0, yl] + r2[k, p, 1, yl]

    def curvature(k, p):
        here = images(p)
        arrived(k, p, 17, r3.at[k, p])
        total = part[k, yl, x, :, here] + r3[k, p]
        pair = total.reshape(2, 2, 8, long)
        prob = jax.nn.sigmoid(pair[:, 0])
        value = prob * (1.0 - prob) * pair[:, 1]
        curv[k, yl, x, :, here] = value.reshape(16, long).astype(bf16)
        mine = curv.at[k, yl, x, :, here]
        for number, device in enumerate((to_yl, to_x_up, to_x_down, *across, to_x_far), 18):
            same(k, p, number, mine, device)

    def terms(k, p):
        if p == 0:
            arrived(k, p, 18, curv.at[k, 1 - yl])
            for number, place in ((19, x_down), (20, x_up), (24, x_far)):
                arrived(k, p, number, curv.at[k, yl, place])
        tile = 1024

        @pl.loop(0, wide // tile)
        def _(n):
            here = pl.ds(pl.multiple_of(p * wide + n * tile, tile), tile)
            term = jnp.dot(
                curv[k].reshape(-1, rows), feat[:, here], preferred_element_type=f32
            )
            hess[k, :, :, :, :, here] = term.reshape(ZS, YHS, CORES, 8, tile)

        there = lanes(p)
        push(k, p, 25, hess.at[k, :, :, 1 - core, :, there], r4.at[k, :, :, :, there], to_core)

    def chip(k, p, place):
        here = lanes(p)
        both = hess[k, place, :, core, :, here] + r4[k, place, :, :, here]
        return both.reshape(16, wide)

    def part_of(k, p, place, half):
        return hess[k, place, half, core, :, lanes(p)] + r4[k, place, half, :, lanes(p)]

    def terms_first(k, p):
        arrived(k, p, 25, r4.at[k, :, :, :, lanes(p)])
        if (k, p) == PAIR_FIRST:
            for place in range(ZS):
                ps[place] = part_of(k, p, place, 1 - yh).astype(bf16)
            push(k, p, 32, ps, pr, to_yh)
            return
        there = ((26, z_far, to_z_far), (28, z_up, to_z_up), (29, z_down, to_z_down))
        for slot, (number, place, device) in enumerate(there):
            zs[k, p, slot] = chip(k, p, place).astype(bf16)
            push(k, p, number, zs.at[k, p, slot], zr.at[k, p, slot], device)

    def terms_second(k, p):
        arrived(k, p, 32, pr)
        there = (
            (30, z_far, to_z_far, theirs_hbm.at[k, :, lanes(p)]),
            (28, z_up, to_z_up, qr.at[0]),
            (29, z_down, to_z_down, qr.at[1]),
        )
        for slot, (number, place, device, dst) in enumerate(there):
            qs[slot] = (part_of(k, p, place, yh) + pr[place].astype(f32)).astype(bf16)
            push(k, p, number, qs.at[slot], dst, device)

    def keep(k, p, value):
        out[k, p] = value
        pltpu.make_async_copy(out.at[k, p], mine_hbm.at[k, :, lanes(p)], store.at[0]).start()

    def terms_pair(k, p):
        if (k, p) == PAIR_FIRST:
            arrived(k, p, 28, qr)
            own = part_of(k, p, z, yh) + pr[z].astype(f32)
            keep(k, p, own + qr[0].astype(f32) + qr[1].astype(f32))
            return
        arrived(k, p, 26, zr.at[k, p])
        own = chip(k, p, z)
        for slot in range(3):
            own = own + zr[k, p, slot].astype(f32)
        first = yh == 0
        ys[k, p] = jnp.where(first, own[8:], own[:8]).astype(bf16)
        push(k, p, 30, ys.at[k, p], theirs_hbm.at[k, :, lanes(p)], to_yh)
        keep(k, p, jnp.where(first, own[:8], own[8:]))

    steps = {one.__name__: one for one in (
        gather_start, gather_second, gather_forward, gather_last, scores, scores_far,
        scores_second, scores_pair, curvature, terms, terms_first, terms_second, terms_pair,
    )}
    loads[0].wait()
    loads[1].wait()
    pack(0)
    pl.semaphore_wait(barrier, len(partners))
    for place, k, p, enough in ORDER:
        for _ in range(min(enough, len(flying))):
            retire()
        steps[NAMES[place]](k, p)
    for k in range(CHUNKS):
        arrived(k, 0, 30, theirs_hbm.at[k])
    pltpu.make_async_copy(mine_hbm, mine_hbm, store.at[0]).wait()
    while flying:
        retire()


def body(features, weights, direction):
    rows, depth = features.shape
    mine = weights.shape[0]
    K, Q = CHUNKS, PIECES
    wide, long = depth // Q, rows // Q
    f32, bf16 = jnp.float32, jnp.bfloat16
    vmem = pltpu.VMEM
    own, other = pl.pallas_call(
        kernel,
        out_shape=(
            jax.ShapeDtypeStruct((K, mine // K, depth), f32),
            jax.ShapeDtypeStruct((K, mine // K, depth), bf16),
        ),
        in_specs=[pl.BlockSpec(memory_space=pl.ANY)] * 3,
        out_specs=[pl.BlockSpec(memory_space=pl.ANY)] * 2,
        scratch_shapes=[
            vmem((rows, depth), bf16),
            vmem((mine, depth), bf16),
            vmem((mine, depth), bf16),
            vmem((K, ZS, YHS, CORES, 16, depth), bf16),
            vmem((K, YLS, XS, 32, rows), f32),
            vmem((K, Q, 32, long), f32),
            vmem((K, Q, 2, 32, long), f32),
            vmem((K, Q, 2, YLS, 32, long), f32),
            vmem((K, Q, 32, long), f32),
            vmem((K, YLS, XS, 16, rows), bf16),
            vmem((K, ZS, YHS, CORES, 8, depth), f32),
            vmem((K, ZS, YHS, 8, depth), f32),
            vmem((K, Q, 3, 16, wide), bf16),
            vmem((K, Q, 3, 16, wide), bf16),
            vmem((K, Q, 8, wide), bf16),
            vmem((K, Q, 8, wide), f32),
            vmem((ZS, 8, wide), bf16),
            vmem((ZS, 8, wide), bf16),
            vmem((3, 8, wide), bf16),
            vmem((2, 8, wide), bf16),
            pltpu.SemaphoreType.DMA((3,)),
            pltpu.SemaphoreType.DMA((1,)),
            pltpu.SemaphoreType.DMA((SENDS,)),
            pltpu.SemaphoreType.DMA((K, Q, 12)),
            pltpu.SemaphoreType.DMA((K, 6)),
            pltpu.SemaphoreType.DMA((K,)),
        ],
        compiler_params=pltpu.CompilerParams(
            collective_id=0, has_side_effects=True, vmem_limit_bytes=62 * 2**20
        ),
    )(features, weights, direction)
    return (4.0 * (own + other.astype(f32))).reshape(mine, depth)


def solution(mesh):
    placed = (P("img", "feat"), P("img", "feat"), P("img", "feat"))
    return jax.shard_map(
        body, mesh=mesh, in_specs=placed, out_specs=P("img", "feat"), check_vma=False
    )
```

```python
import jax
import jax.numpy as jnp
from jax import lax
from jax.experimental import pallas as pl
from jax.experimental.pallas import tpu as pltpu
from jax.sharding import PartitionSpec as P

ZS, YHS, CORES, YLS, XS = 4, 2, 2, 2, 4
CHUNKS = 4
PIECES = 2
BY_PIECE = {0: 0, 1: 1, 3: 1, 2: 2, 4: 2, 5: 3, 6: 4, 13: 5, 14: 6, 15: 7, 16: 7, 17: 8}
BY_PIECE |= {25: 9, 26: 10, 28: 10, 29: 10, 31: 11}
BY_CHUNK = {7: 0, 8: 0, 9: 0, 10: 0, 11: 0, 12: 0, 18: 1, 21: 1, 22: 1, 23: 1, 19: 2, 20: 3, 24: 4}
BY_CHUNK |= {32: 5}
SENDS = 48
PAIRED = (1, 2, 3)
PAIR_FIRST = (3, 1)
RING_FIRST = (0, 1)
NAMES = (
    "gather_start", "gather_second", "gather_forward", "gather_last",
    "scores", "scores_far", "scores_second", "scores_pair", "curvature", "", "",
    "terms", "terms_first", "terms_second", "terms_pair",
)
ORDER = (
    (0, 0, 0, 0), (0, 1, 1, 0), (0, 0, 1, 0), (0, 1, 0, 0), (1, 0, 0, 0), (1, 0, 1, 0),
    (1, 1, 1, 0), (1, 1, 0, 8), (2, 0, 1, 4), (2, 0, 0, 0), (2, 1, 1, 7), (2, 1, 0, 4),
    (0, 2, 1, 0), (0, 2, 0, 0), (3, 0, 1, 5), (3, 0, 0, 3), (4, 0, 0, 2), (3, 1, 0, 6),
    (3, 1, 1, 0), (0, 3, 0, 0), (4, 0, 1, 0), (1, 2, 0, 0), (4, 1, 0, 0), (1, 2, 1, 0),
    (6, 0, 0, 10), (4, 1, 1, 0), (2, 2, 0, 14), (5, 1, 0, 0), (6, 0, 1, 0), (2, 2, 1, 6),
    (1, 3, 0, 0), (5, 1, 1, 0), (0, 3, 1, 0), (6, 1, 0, 4), (7, 0, 0, 0), (3, 2, 0, 1),
    (3, 2, 1, 5), (1, 3, 1, 0), (7, 0, 1, 6), (6, 1, 1, 0), (4, 2, 0, 0), (2, 3, 0, 0),
    (4, 2, 1, 0), (8, 0, 0, 0), (2, 3, 1, 0), (5, 2, 0, 15), (7, 1, 0, 0), (8, 0, 1, 0),
    (3, 3, 0, 4), (5, 2, 1, 7), (3, 3, 1, 0), (7, 1, 1, 0), (6, 2, 0, 7), (4, 3, 0, 0),
    (6, 2, 1, 14), (4, 3, 1, 0), (11, 0, 0, 0), (5, 3, 0, 14), (8, 1, 1, 0), (11, 0, 1, 0),
    (5, 3, 1, 3), (8, 1, 0, 0), (12, 0, 0, 0), (7, 2, 0, 0), (6, 3, 0, 1), (7, 2, 1, 0),
    (6, 3, 1, 4), (8, 2, 1, 10), (8, 2, 0, 0), (12, 0, 1, 0), (7, 3, 0, 13), (11, 1, 0, 0),
    (11, 1, 1, 0), (7, 3, 1, 3), (12, 1, 0, 0), (8, 3, 0, 0), (12, 1, 1, 0), (8, 3, 1, 5),
    (11, 2, 0, 0), (11, 2, 1, 0), (12, 2, 0, 19), (11, 3, 0, 9), (11, 3, 1, 0), (12, 2, 1, 0),
    (14, 1, 0, 0), (12, 3, 1, 11), (12, 3, 0, 0), (14, 0, 1, 0), (14, 0, 0, 0), (14, 1, 1, 0),
    (14, 2, 1, 2), (13, 3, 1, 5), (14, 2, 0, 0), (14, 3, 0, 2), (14, 3, 1, 0),
)


def kernel(
    feat_hbm, w_hbm, d_hbm, mine_hbm, theirs_hbm,
    feat, w_ref, d_ref, gath, part, rf, r1, r2, r3, curv, hess, r4,
    zs, zr, ys, out, ps, pr, qs, qr,
    load, store, send, by_piece, by_chunk, last,
):
    f32, bf16 = jnp.float32, jnp.bfloat16
    mesh_ids = pl.DeviceIdType.MESH
    img, col = lax.axis_index("img"), lax.axis_index("feat")
    core = lax.rem(img, CORES)
    yh = lax.rem(img // CORES, YHS)
    z = img // (CORES * YHS)
    x = lax.rem(col, XS)
    yl = col // XS
    z_up, z_down, z_far = lax.rem(z + 1, ZS), lax.rem(z + 3, ZS), lax.rem(z + 2, ZS)
    x_up, x_down, x_far = lax.rem(x + 1, XS), lax.rem(x + 3, XS), lax.rem(x + 2, XS)

    def at(z=z, yh=yh, core=core, yl=yl, x=x):
        return {"img": (z * YHS + yh) * CORES + core, "feat": yl * XS + x}

    to_z_up, to_z_down, to_z_far = at(z=z_up), at(z=z_down), at(z=z_far)
    to_x_up, to_x_down, to_x_far = at(x=x_up), at(x=x_down), at(x=x_far)
    to_yh, to_core, to_yl = at(yh=1 - yh), at(core=1 - core), at(yl=1 - yl)
    across = [at(yl=1 - yl, x=one) for one in (x_up, x_down, x_far)]

    loads = [
        pltpu.make_async_copy(w_hbm, w_ref, load.at[0]),
        pltpu.make_async_copy(d_hbm, d_ref, load.at[1]),
        pltpu.make_async_copy(feat_hbm, feat, load.at[2]),
    ]
    for one in loads:
        one.start()
    barrier = pltpu.get_barrier_semaphore()
    partners = [
        to_core, to_yl, to_z_up, to_z_down, to_x_up, to_x_down,
        to_yh,
    ]
    for partner in partners:
        pl.semaphore_signal(barrier, inc=1, device_id=partner, device_id_type=mesh_ids)

    rows, depth = feat.shape
    wide, long = depth // PIECES, rows // PIECES
    slots, flying, waiting = list(range(SENDS)), [], [loads[2]]
    unpacked = list(range(1, CHUNKS))

    def lanes(p):
        return pl.ds(p * wide, wide)

    def images(p):
        return pl.ds(p * long, long)

    def receive(k, p, number):
        if number in BY_PIECE:
            return by_piece.at[k, p, BY_PIECE[number]]
        return by_chunk.at[k, BY_CHUNK[number]] if number in BY_CHUNK else last.at[k]

    def retire():
        slot, one = flying.pop(0)
        one.wait_send()
        slots.append(slot)

    def push(k, p, number, src, dst, device):
        if not slots:
            retire()
        slot = slots.pop(0)
        one = pltpu.make_async_remote_copy(
            src_ref=src,
            dst_ref=dst,
            send_sem=send.at[slot],
            recv_sem=receive(k, p, number),
            device_id=device,
            device_id_type=mesh_ids,
        )
        one.start()
        flying.append((slot, one))

    def arrived(k, p, number, ref):
        pltpu.make_async_remote_copy(
            src_ref=ref,
            dst_ref=ref,
            send_sem=send.at[0],
            recv_sem=receive(k, p, number),
            device_id=to_core,
            device_id_type=mesh_ids,
        ).wait_recv()

    def same(k, p, number, ref, device):
        push(k, p, number, ref, ref, device)

    def pack(k):
        both = jnp.concatenate(
            (
                w_ref[...].astype(f32)[8 * k : 8 * k + 8],
                d_ref[...].astype(f32)[8 * k : 8 * k + 8],
            ),
            axis=0,
        )
        gath[k, z, yh, core] = both.astype(bf16)

    def gather_start(k, p):
        if k in unpacked:
            unpacked.remove(k)
            pack(k)
        mine = gath.at[k, z, yh, core, :, lanes(p)]
        same(k, p, 1, mine, to_z_up)
        same(k, p, 2, mine, to_z_down)
        same(k, p, 0, mine, to_yh)
        same(k, p, 7, mine, to_core)

    def ring_second(k, p):
        half = wide // 2
        down = gath.at[k, z_down, yh, core]
        arrived(k, p, 1, down.at[:, lanes(p)])
        same(k, p, 5, down.at[:, pl.ds(p * wide, half)], to_z_up)
        same(k, p, 0, down.at[:, lanes(p)], to_yh)
        same(k, p, 9, down.at[:, lanes(p)], to_core)
        up = gath.at[k, z_up, yh, core]
        arrived(k, p, 2, up.at[:, lanes(p)])
        same(k, p, 6, up.at[:, pl.ds(p * wide + half, half)], to_z_down)
        same(k, p, 0, up.at[:, lanes(p)], to_yh)
        same(k, p, 10, up.at[:, lanes(p)], to_core)

    def ring_forward(k, p):
        half = wide // 2
        far = gath.at[k, z_far, yh, core]
        arrived(k, p, 5, far.at[:, pl.ds(p * wide, half)])
        arrived(k, p, 6, far.at[:, pl.ds(p * wide + half, half)])
        same(k, p, 0, far.at[:, lanes(p)], to_yh)
        same(k, p, 11, far.at[:, lanes(p)], to_core)

    def ring_last(k, p):
        theirs = gath.at[k, :, 1 - yh, core, :, lanes(p)]
        arrived(k, p, 0, theirs)
        same(k, p, 12, theirs, to_core)

    def gather_second(k, p):
        if (k, p) == RING_FIRST:
            return ring_second(k, p)
        theirs = gath.at[k, z, 1 - yh, core, :, lanes(p)]
        arrived(k, p, 0, theirs)
        same(k, p, 3, theirs, to_z_up)
        same(k, p, 4, theirs, to_z_down)
        same(k, p, 8, theirs, to_core)

    def gather_forward(k, p):
        if (k, p) == RING_FIRST:
            return ring_forward(k, p)
        arrived(k, p, 1, gath.at[k, z_down, :, core, :, lanes(p)])
        same(k, p, 5, gath.at[k, z_down, 0, core, :, lanes(p)], to_z_up)
        arrived(k, p, 2, gath.at[k, z_up, :, core, :, lanes(p)])
        same(k, p, 6, gath.at[k, z_up, 1, core, :, lanes(p)], to_z_down)
        same(k, p, 9, gath.at[k, z_down, :, core, :, lanes(p)], to_core)
        same(k, p, 10, gath.at[k, z_up, :, core, :, lanes(p)], to_core)

    def gather_last(k, p):
        if (k, p) == RING_FIRST:
            return ring_last(k, p)
        arrived(k, p, 5, gath.at[k, z_far, 0, core, :, lanes(p)])
        same(k, p, 11, gath.at[k, z_far, 0, core, :, lanes(p)], to_core)
        arrived(k, p, 6, gath.at[k, z_far, 1, core, :, lanes(p)])
        same(k, p, 12, gath.at[k, z_far, 1, core, :, lanes(p)], to_core)

    def scores(k, p):
        here = images(p)
        if waiting:
            waiting.pop().wait()
        if p == 0:
            arrived(k, p, 7, gath.at[k, :, :, 1 - core])
        both = lax.dot_general(
            gath[k].reshape(-1, depth),
            feat[here, :],
            (((1,), (1,)), ((), ())),
            preferred_element_type=f32,
        )
        part[k, :, :, :, here] = both.reshape(YLS, XS, -1, long)
        if k in PAIRED:
            push(k, p, 31, part.at[k, 1 - yl, x_far, :, here], rf.at[k, p], to_yl)
        else:
            push(k, p, 13, part.at[k, 0, x_far, :, here], r1.at[k, p, 0], to_x_up)
            push(k, p, 14, part.at[k, 1, x_far, :, here], r1.at[k, p, 1], to_x_down)

    def halves(p):
        half = long // 2
        return pl.ds(p * long, half), pl.ds(p * long + half, half), pl.ds(0, half)

    def scores_far(k, p):
        first, second, slot = halves(p)
        arrived(k, p, 31, rf.at[k, p])
        part[k, yl, x_far, :, images(p)] += rf[k, p]
        push(k, p, 13, part.at[k, yl, x_far, :, first], r1.at[k, p, 0, :, slot], to_x_up)
        push(k, p, 14, part.at[k, yl, x_far, :, second], r1.at[k, p, 1, :, slot], to_x_down)

    def scores_second(k, p):
        here = images(p)
        first, second, slot = halves(p)
        up = r1.at[k, p, 0, :, slot] if k in PAIRED else r1.at[k, p, 0]
        down = r1.at[k, p, 1, :, slot] if k in PAIRED else r1.at[k, p, 1]
        arrived(k, p, 13, up)
        if k in PAIRED:
            part[k, yl, x_up, :, first] += r1[k, p, 0, :, slot]
        else:
            part[k, 0, x_up, :, here] += r1[k, p, 0]
        push(k, p, 15, part.at[k, :, x_up, :, here], r2.at[k, p, 0], to_x_up)
        arrived(k, p, 14, down)
        if k in PAIRED:
            part[k, yl, x_down, :, second] += r1[k, p, 1, :, slot]
        else:
            part[k, 1, x_down, :, here] += r1[k, p, 1]
        push(k, p, 16, part.at[k, :, x_down, :, here], r2.at[k, p, 1], to_x_down)

    def scores_pair(k, p):
        here = images(p)
        arrived(k, p, 15, r2.at[k, p])
        part[k, 1 - yl, x, :, here] += r2[k, p, 0, 1 - yl] + r2[k, p, 1, 1 - yl]
        push(k, p, 17, part.at[k, 1 - yl, x, :, here], r3.at[k, p], to_yl)
        part[k, yl, x, :, here] += r2[k, p, 0, yl] + r2[k, p, 1, yl]

    def curvature(k, p):
        here = images(p)
        arrived(k, p, 17, r3.at[k, p])
        total = part[k, yl, x, :, here] + r3[k, p]
        pair = total.reshape(2, 2, 8, long)
        prob = jax.nn.sigmoid(pair[:, 0])
        value = prob * (1.0 - prob) * pair[:, 1]
        curv[k, yl, x, :, here] = value.reshape(16, long).astype(bf16)
        mine = curv.at[k, yl, x, :, here]
        for number, device in enumerate((to_yl, to_x_up, to_x_down, *across, to_x_far), 18):
            same(k, p, number, mine, device)

    def terms(k, p):
        if p == 0:
            arrived(k, p, 18, curv.at[k, 1 - yl])
            for number, place in ((19, x_down), (20, x_up), (24, x_far)):
                arrived(k, p, number, curv.at[k, yl, place])
        tile = 1024

        @pl.loop(0, wide // tile)
        def _(n):
            here = pl.ds(pl.multiple_of(p * wide + n * tile, tile), tile)
            term = jnp.dot(
                curv[k].reshape(-1, rows), feat[:, here], preferred_element_type=f32
            )
            hess[k, :, :, :, :, here] = term.reshape(ZS, YHS, CORES, 8, tile)

        there = lanes(p)
        push(k, p, 25, hess.at[k, :, :, 1 - core, :, there], r4.at[k, :, :, :, there], to_core)

    def chip(k, p, place):
        here = lanes(p)
        both = hess[k, place, :, core, :, here] + r4[k, place, :, :, here]
        return both.reshape(16, wide)

    def part_of(k, p, place, half):
        return hess[k, place, half, core, :, lanes(p)] + r4[k, place, half, :, lanes(p)]

    def terms_first(k, p):
        arrived(k, p, 25, r4.at[k, :, :, :, lanes(p)])
        if (k, p) == PAIR_FIRST:
            for place in range(ZS):
                ps[place] = part_of(k, p, place, 1 - yh).astype(bf16)
            push(k, p, 32, ps, pr, to_yh)
            return
        there = ((26, z_far, to_z_far), (28, z_up, to_z_up), (29, z_down, to_z_down))
        for slot, (number, place, device) in enumerate(there):
            zs[k, p, slot] = chip(k, p, place).astype(bf16)
            push(k, p, number, zs.at[k, p, slot], zr.at[k, p, slot], device)

    def terms_second(k, p):
        arrived(k, p, 32, pr)
        there = (
            (30, z_far, to_z_far, theirs_hbm.at[k, :, lanes(p)]),
            (28, z_up, to_z_up, qr.at[0]),
            (29, z_down, to_z_down, qr.at[1]),
        )
        for slot, (number, place, device, dst) in enumerate(there):
            qs[slot] = (part_of(k, p, place, yh) + pr[place].astype(f32)).astype(bf16)
            push(k, p, number, qs.at[slot], dst, device)

    def keep(k, p, value):
        out[k, p] = value
        pltpu.make_async_copy(out.at[k, p], mine_hbm.at[k, :, lanes(p)], store.at[0]).start()

    def terms_pair(k, p):
        if (k, p) == PAIR_FIRST:
            arrived(k, p, 28, qr)
            own = part_of(k, p, z, yh) + pr[z].astype(f32)
            keep(k, p, own + qr[0].astype(f32) + qr[1].astype(f32))
            return
        arrived(k, p, 26, zr.at[k, p])
        own = chip(k, p, z)
        for slot in range(3):
            own = own + zr[k, p, slot].astype(f32)
        first = yh == 0
        ys[k, p] = jnp.where(first, own[8:], own[:8]).astype(bf16)
        push(k, p, 30, ys.at[k, p], theirs_hbm.at[k, :, lanes(p)], to_yh)
        keep(k, p, jnp.where(first, own[:8], own[8:]))

    steps = {one.__name__: one for one in (
        gather_start, gather_second, gather_forward, gather_last, scores, scores_far,
        scores_second, scores_pair, curvature, terms, terms_first, terms_second, terms_pair,
    )}
    loads[0].wait()
    loads[1].wait()
    pack(0)
    pl.semaphore_wait(barrier, len(partners))
    for place, k, p, enough in ORDER:
        for _ in range(min(enough, len(flying))):
            retire()
        steps[NAMES[place]](k, p)
    for k in range(CHUNKS):
        arrived(k, 0, 30, theirs_hbm.at[k])
    pltpu.make_async_copy(mine_hbm, mine_hbm, store.at[0]).wait()
    while flying:
        retire()


def body(features, weights, direction):
    rows, depth = features.shape
    mine = weights.shape[0]
    K, Q = CHUNKS, PIECES
    wide, long = depth // Q, rows // Q
    f32, bf16 = jnp.float32, jnp.bfloat16
    vmem = pltpu.VMEM
    own, other = pl.pallas_call(
        kernel,
        out_shape=(
            jax.ShapeDtypeStruct((K, mine // K, depth), f32),
            jax.ShapeDtypeStruct((K, mine // K, depth), bf16),
        ),
        in_specs=[pl.BlockSpec(memory_space=pl.ANY)] * 3,
        out_specs=[pl.BlockSpec(memory_space=pl.ANY)] * 2,
        scratch_shapes=[
            vmem((rows, depth), bf16),
            vmem((mine, depth), bf16),
            vmem((mine, depth), bf16),
            vmem((K, ZS, YHS, CORES, 16, depth), bf16),
            vmem((K, YLS, XS, 32, rows), f32),
            vmem((K, Q, 32, long), f32),
            vmem((K, Q, 2, 32, long), f32),
            vmem((K, Q, 2, YLS, 32, long), f32),
            vmem((K, Q, 32, long), f32),
            vmem((K, YLS, XS, 16, rows), bf16),
            vmem((K, ZS, YHS, CORES, 8, depth), f32),
            vmem((K, ZS, YHS, 8, depth), f32),
            vmem((K, Q, 3, 16, wide), bf16),
            vmem((K, Q, 3, 16, wide), bf16),
            vmem((K, Q, 8, wide), bf16),
            vmem((K, Q, 8, wide), f32),
            vmem((ZS, 8, wide), bf16),
            vmem((ZS, 8, wide), bf16),
            vmem((3, 8, wide), bf16),
            vmem((2, 8, wide), bf16),
            pltpu.SemaphoreType.DMA((3,)),
            pltpu.SemaphoreType.DMA((1,)),
            pltpu.SemaphoreType.DMA((SENDS,)),
            pltpu.SemaphoreType.DMA((K, Q, 12)),
            pltpu.SemaphoreType.DMA((K, 6)),
            pltpu.SemaphoreType.DMA((K,)),
        ],
        compiler_params=pltpu.CompilerParams(
            collective_id=0, has_side_effects=True, vmem_limit_bytes=62 * 2**20
        ),
    )(features, weights, direction)
    return (4.0 * (own + other.astype(f32))).reshape(mine, depth)


def solution(mesh):
    placed = (P("img", "feat"), P("img", "feat"), P("img", "feat"))
    return jax.shard_map(
        body, mesh=mesh, in_specs=placed, out_specs=P("img", "feat"), check_vma=False
    )
```
